32 devices in a mesh: patch: 16 (over z, y, core), lev: 2 (over x).
Axes of the slice: x: 2, y: 2, z: 4, core: 2. Of those that a mesh axis runs over, the one named last changes fastest.
Arguments:
- fields: float32 [3, 24, 32768], P(None, 'lev', 'patch'), may hold values from -6 to 6
- stencil_index: int32 [12, 2, 32768], P(None, 'lev', 'patch'), may hold values from 0 to 3071, as said below
- stencil_weight: float32 [12, 2, 32768], P(None, 'lev', 'patch'), may hold values from -0.2 to 0.4
- neighbours: int32 [6, 32768], P(None, 'patch'), may hold values from 0 to 2175, as said below
- lap_weight: float32 [6, 32768], P(None, 'patch'), may hold values from 0.2 to 1
- edge_x: float32 [6, 32768], P(None, 'patch'), may hold values from -1.8 to 1.8
- edge_y: float32 [6, 32768], P(None, 'patch'), may hold values from -1.8 to 1.8
- to_modes: float32 [24, 24], replicated, may hold values from -1.25 to 1.25
- from_modes: float32 [24, 24], replicated, may hold values from -1.25 to 1.25
- helm_coef: float32 [24], P('lev'), may hold values from 0.15 to 0.6
Outputs:
- new_winds: float32 [2, 24, 32768], P(None, 'lev', 'patch')
- new_height: float32 [24, 32768], P('lev', 'patch')
The draws below stay inside these ranges and needn't reach their ends.
Inputs may be any that keep to these rules, and one draw needn't show every extreme that they name: `stencil_index`: entry [p, g, i] is a position in the cells of i's patch extended by 512 cells on each side along the closed chain; position 512 + (i mod 2048) is cell i itself, and the entry lies at most 512 from it. `neighbours`: entry [k, i] is a position in the cells of i's patch extended by 64 cells on each side along the closed chain; position 64 + (i mod 2048) is cell i itself, which is never named.
All inputs are finite; a program needn't handle non-finite values.
Results may differ from the reference program's by a relative error of at most 0.000096.
Values sent between devices are 32-bit elements; how exact they have to be, the bound alone decides.
A program may use at most 64 MiB of HBM per device.

```python
import math
import jax
import jax.numpy as jnp
from jax import lax

CELLS_DEV = 2048
LEV_DEV = 12
REACH = 512
NBR_REACH = 64
SWEEPS = 4
LEVELS = 24
GROUPS = 2
NCELLS = 32768


def draw_stencil_index(key, part):
    key_reach = jax.random.fold_in(key, 11)
    key_group = jax.random.fold_in(key, 12)
    key_patch = jax.random.fold_in(key, 13)
    key_shift = jax.random.fold_in(key, 14)
    key_spread = jax.random.fold_in(key, 15)
    patches = NCELLS // CELLS_DEV
    reach_block = jax.random.randint(key_reach, (GROUPS, patches), 4, REACH + 1)
    group_pick = jax.random.randint(key_group, (), 0, GROUPS)
    patch_pick = jax.random.randint(key_patch, (), 0, patches)
    reach_block = reach_block.at[group_pick, patch_pick].set(REACH)
    reach_cell = jnp.repeat(reach_block, CELLS_DEV, axis=1)
    centre = REACH + jnp.arange(NCELLS, dtype=jnp.int32) % CELLS_DEV
    displace = jax.random.randint(key_shift, (GROUPS, NCELLS), -(reach_cell - 3), reach_cell - 2)
    spread = jax.random.randint(key_spread, (12, GROUPS, NCELLS), -3, 4)
    position = centre[None, None, :] + displace[None] + spread
    position = jnp.clip(position, centre[None, None, :] - reach_cell[None], centre[None, None, :] + reach_cell[None])
    first_cell = patch_pick * CELLS_DEV
    position = position.at[0, group_pick, first_cell].set(0)
    position = position.at[1, group_pick, first_cell + CELLS_DEV - 1].set(2 * REACH + CELLS_DEV - 1)
    return position.astype(jnp.int32)


def draw_neighbours(key, part):
    key_distance = jax.random.fold_in(key, 21)
    key_direction = jax.random.fold_in(key, 22)
    key_patch = jax.random.fold_in(key, 23)
    patches = NCELLS // CELLS_DEV
    distance = jax.random.randint(key_distance, (6, NCELLS), 1, NBR_REACH + 1)
    direction = jax.random.randint(key_direction, (6, NCELLS), 0, 2) * 2 - 1
    centre = NBR_REACH + jnp.arange(NCELLS, dtype=jnp.int32) % CELLS_DEV
    position = centre[None, :] + direction * distance
    patch_pick = jax.random.randint(key_patch, (), 0, patches)
    first_cell = patch_pick * CELLS_DEV
    position = position.at[0, first_cell].set(0)
    position = position.at[1, first_cell + CELLS_DEV - 1].set(2 * NBR_REACH + CELLS_DEV - 1)
    return position.astype(jnp.int32)


def steps_of(key, dims, cuts, least, high):
    factor_of, own = 1.0, jax.random.fold_in(key, 6)
    for dim, blocks in cuts:
        steps = jnp.exp(jax.random.uniform(jax.random.fold_in(own, dim), (blocks,), jnp.float32, least / len(cuts), high / len(cuts)))
        factor_of = factor_of * jnp.repeat(steps, dims[dim] // blocks).reshape([-1 if axis == dim else 1 for axis in range(len(dims))])
    return factor_of


def gaussian(rng, shape, scale, most, shards=(), held_as=jnp.bfloat16):
    loudness = steps_of(rng, shape, shards, -0.22, 0.18) if shards else 1.0
    drawn = jax.random.normal(rng, shape, jnp.float32) * scale * loudness
    return jnp.minimum(jnp.maximum(drawn, -most), most).astype(held_as)


def setup_inputs(seed: int = 0) -> dict:
    splits = jax.random.split(jax.random.key(seed), 11)
    fields = gaussian(splits[0], (3, LEVELS, NCELLS), 1.0, 6.0, ((1, 2), (2, 16)), jnp.float32)
    stencil_index = draw_stencil_index(jax.random.fold_in(splits[10], 71), 0)
    stencil_weight = jnp.clip(-0.2 + 0.6 * jax.random.uniform(splits[2], (12, GROUPS, NCELLS), jnp.float32) ** steps_of(splits[2], (12, GROUPS, NCELLS), ((1, 2), (2, 16)), -0.2, 0.2), -0.2, 0.4)
    neighbours = draw_neighbours(jax.random.fold_in(splits[10], 71), 0)
    lap_weight = jnp.clip(0.2 + 0.8 * jax.random.uniform(splits[4], (6, NCELLS), jnp.float32) ** steps_of(splits[4], (6, NCELLS), ((1, 16),), -0.2, 0.2), 0.2, 1.0)
    edge_x = gaussian(splits[5], (6, NCELLS), 0.3, 1.8, ((1, 16),), jnp.float32)
    edge_y = gaussian(splits[6], (6, NCELLS), 0.3, 1.8, ((1, 16),), jnp.float32)
    to_modes = gaussian(splits[7], (LEVELS, LEVELS), LEVELS ** -0.5, 1.25, (), jnp.float32)
    from_modes = gaussian(splits[8], (LEVELS, LEVELS), LEVELS ** -0.5, 1.25, (), jnp.float32)
    helm_coef = jnp.clip(jnp.exp(math.log(0.6) - 1.3862944 * jax.random.uniform(splits[9], (LEVELS,), jnp.float32) ** steps_of(splits[9], (LEVELS,), ((0, 2),), -0.2, 0.2)), 0.15, 0.6)
    return dict(fields=fields, stencil_index=stencil_index, stencil_weight=stencil_weight, neighbours=neighbours, lap_weight=lap_weight, edge_x=edge_x, edge_y=edge_y, to_modes=to_modes, from_modes=from_modes, helm_coef=helm_coef)


coupling = 0.5


def reference(fields, stencil_index, stencil_weight, neighbours, lap_weight, edge_x, edge_y, to_modes, from_modes, helm_coef):
    cell_ids = jnp.arange(NCELLS, dtype=jnp.int32)
    block_start = (cell_ids // CELLS_DEV) * CELLS_DEV
    source = (block_start + stencil_index - REACH) % NCELLS
    grouped = fields.reshape(3, GROUPS, LEV_DEV, NCELLS)
    upstream = jnp.zeros((3, GROUPS, LEV_DEV, NCELLS), jnp.float32)
    for point_no in range(12):
        taken = jnp.take_along_axis(grouped, source[point_no][None, :, None, :].astype(jnp.int32), axis=3)
        upstream = upstream + stencil_weight[point_no][None, :, None, :] * taken
    upstream = upstream.reshape(3, LEVELS, NCELLS)
    new_winds = upstream[0:2]
    beside_ids = (block_start + neighbours - NBR_REACH) % NCELLS
    divergence = jnp.zeros((LEVELS, NCELLS), jnp.float32)
    for slot_no in range(6):
        across = upstream[0][:, beside_ids[slot_no]] - upstream[0]
        along = upstream[1][:, beside_ids[slot_no]] - upstream[1]
        divergence = divergence + edge_x[slot_no] * across + edge_y[slot_no] * along
    right_side = upstream[2] - coupling * divergence
    modal_rhs = jnp.dot(to_modes, right_side, precision=lax.Precision.HIGHEST, preferred_element_type=jnp.float32)
    stiffness = helm_coef[:, None]
    weight_sum = jnp.sum(lap_weight, axis=0)
    diagonal = 1.0 + stiffness * weight_sum[None, :]
    radius = 6.0 * stiffness / (1.0 + 6.0 * stiffness)
    iterate = jnp.zeros((LEVELS, NCELLS), jnp.float32)
    for sweep_no in range(SWEEPS):
        step_size = 1.0 / (1.0 + radius * jnp.cos(jnp.pi * (2 * sweep_no + 1) / (2.0 * SWEEPS)))
        laplace = jnp.zeros((LEVELS, NCELLS), jnp.float32)
        for slot_no in range(6):
            laplace = laplace + lap_weight[slot_no] * (iterate[:, beside_ids[slot_no]] - iterate)
        applied = iterate - stiffness * laplace
        iterate = iterate + step_size * (modal_rhs - applied) / diagonal
    new_height = jnp.dot(from_modes, iterate, precision=lax.Precision.HIGHEST, preferred_element_type=jnp.float32)
    return new_winds, new_height
```

```python
import functools
import math

import jax
import jax.numpy as jnp
from jax import lax
from jax.experimental import pallas as pl
from jax.experimental.pallas import tpu as pltpu
from jax.sharding import PartitionSpec as P

REACH = 512
NBR_REACH = 64
SWEEPS = 4
COUPLING = 0.5
LANES = 128
SUB = 8
HALO = NBR_REACH * SWEEPS
FIELD_HALO = REACH + HALO
MESH = pl.DeviceIdType.MESH


def up8(rows):
    return -(-rows // SUB) * SUB


def lanes_of(x, index):
    return jnp.take_along_axis(x, index, axis=1, mode="promise_in_bounds")


def row8(ref, row, cols):
    return jnp.broadcast_to(ref[pl.ds(row, 1), cols], (SUB, LANES))


def cols_of(block):
    return pl.ds(pl.multiple_of(block * LANES, LANES), LANES)


def loop(first, last, body, unroll=1):
    count = last - first
    while count % unroll:
        unroll -= 1

    def step(i, carry):
        for u in range(unroll):
            body(first + i * unroll + u)
        return carry

    lax.fori_loop(0, count // unroll, step, 0)


def kernel(
    npatch, nlev,
    fields_in, s_index_in, s_weight_in, nbr_in, lap_in, ex_in, ey_in, to_modes, from_modes, helm,
    winds_out, height_out,
    fields, s_index, s_weight, nbr, lap, ex, ey, winds, load_sem, wind_sem,
    f_halo, si_halo, sw_halo, nb_halo, lw_halo, ex_halo, ey_halo, hc,
    F, G0, G1, si, sw, nb, lw, gx, gy, U, rx, rinv, cinv, xa, xb, to_wide, from_wide,
    send_sem, recv_sem, lev_send, lev_recv, hc_send, hc_recv,
):
    group = fields.shape[1]
    cells = fields.shape[2]
    levels = group * nlev
    points = s_index.shape[0]
    sides = nbr.shape[0]
    ext = cells + 2 * HALO
    nb_blocks = ext // LANES
    hb = HALO // LANES
    patch = lax.axis_index("patch")
    lev = lax.axis_index("lev")
    right = lax.rem(patch + 1, npatch)
    left = lax.rem(patch + npatch - 1, npatch)

    barrier = pltpu.get_barrier_semaphore()
    for to in (left, right):
        pl.semaphore_signal(barrier, inc=1, device_id={"patch": to}, device_id_type=MESH)
    for d in range(1, nlev):
        pl.semaphore_signal(
            barrier, inc=1, device_id={"lev": lax.rem(lev + d, nlev)}, device_id_type=MESH
        )
    loads = []
    for no, (src, dst) in enumerate((
        (fields_in, fields), (s_index_in, s_index), (s_weight_in, s_weight),
        (nbr_in, nbr), (lap_in, lap), (ex_in, ex), (ey_in, ey),
    )):
        copy = pltpu.make_async_copy(src, dst, load_sem.at[no])
        copy.start()
        loads.append(copy)

    hc[lev] = helm[...]
    back = from_modes[0:group, :]
    for g in range(1, nlev):
        back = jnp.where(lev == g, from_modes[g * group : (g + 1) * group, :], back)
    for m in range(levels):
        to_wide[m, 0:levels] = jnp.broadcast_to(to_modes[:, m : m + 1], (levels, LANES))
        from_wide[m, 0:group] = jnp.broadcast_to(back[:, m : m + 1], (group, LANES))
    for copy in loads:
        copy.wait()
    pl.semaphore_wait(barrier, 2 + nlev - 1)

    copies = []
    pairs = (
        (fields, f_halo, FIELD_HALO),
        (s_index, si_halo, HALO),
        (s_weight, sw_halo, HALO),
        (nbr, nb_halo, HALO),
        (lap, lw_halo, HALO),
        (ex, ex_halo, HALO),
        (ey, ey_halo, HALO),
    )
    for no, (src, dst, width) in enumerate(pairs):
        lead = (slice(None),) * (len(src.shape) - 1)
        for side in (0, 1):
            start = cells - width if side == 0 else 0
            copy = pltpu.make_async_remote_copy(
                src_ref=src.at[lead + (pl.ds(start, width),)],
                dst_ref=dst.at[side],
                send_sem=send_sem.at[2 * no + side],
                recv_sem=recv_sem.at[2 * no + side],
                device_id={"patch": right if side == 0 else left},
                device_id_type=MESH,
            )
            copy.start()
            copies.append(copy)
    hc_copies = []
    for d in range(1, nlev):
        copy = pltpu.make_async_remote_copy(
            src_ref=helm,
            dst_ref=hc.at[lev],
            send_sem=hc_send.at[d - 1],
            recv_sem=hc_recv.at[d - 1],
            device_id={"lev": lax.rem(lev + d, nlev)},
            device_id_type=MESH,
        )
        copy.start()
        hc_copies.append(copy)

    for f in range(3):
        F[f * group : (f + 1) * group, FIELD_HALO : FIELD_HALO + cells] = fields[f]
    own = slice(HALO, HALO + cells)
    si[:, own] = s_index[:, 0, :] + HALO
    sw[:, own] = s_weight[:, 0, :]
    nb[:, own] = nbr[...] + (HALO - NBR_REACH)
    lw[:, own] = lap[...]
    gx[:, own] = ex[...]
    gy[:, own] = ey[...]

    frows = F.shape[0]
    tiles = 2 * REACH // LANES + 1
    ftiles = F.shape[1] // LANES
    own_lo = FIELD_HALO // LANES
    own_hi = own_lo + cells // LANES

    def split_tiles(first_tile, last_tile, to):
        base = first_tile * frows + (frows if first_tile % 2 else 0) % (2 * SUB)
        rows = 2 * frows
        for no, tile in enumerate(range(first_tile, last_tile, 2)):
            pair = [
                F[:, min(t, ftiles - 1) * LANES : (min(t, ftiles - 1) + 1) * LANES]
                for t in (tile, tile + 1)
            ]
            x = jnp.concatenate(pair, axis=0)
            high = x.astype(jnp.bfloat16)
            at = slice(base + no * rows, base + (no + 1) * rows)
            to[at, 0:LANES] = high
            to[at, LANES : 2 * LANES] = (x - high.astype(jnp.float32)).astype(jnp.bfloat16)

    split_tiles(own_lo, own_hi, G0)
    split_tiles(own_lo + 1, own_hi, G1)
    lane_id = lax.broadcasted_iota(jnp.int32, (LANES, LANES), 0).astype(jnp.float32).astype(jnp.bfloat16)
    one = jnp.ones((LANES, LANES), jnp.bfloat16)
    zero = jnp.zeros((LANES, LANES), jnp.bfloat16)

    by_product = points - 2 * (points // 6)

    def upstream(b, odd):
        cols = cols_of(b)
        acc = [None] * (frows // SUB)
        start = pl.multiple_of(b * frows + (frows if odd else 0) % (2 * SUB), 2 * SUB)
        field = (G1 if odd else G0)[pl.ds(start, tiles * frows), :]
        for p in range(0, points, 2):
            pair = (p, p + 1)
            his, los = [], []
            for q in pair:
                x = row8(si, q, cols)
                his.append((x >> (LANES.bit_length() - 1)) - b)
                los.append(x & (LANES - 1))
            if p < by_product:
                hot = []
                for lo in los:
                    lo = jnp.broadcast_to(lo[0:1].astype(jnp.float32), (LANES, LANES))
                    h = jnp.where(lane_id == lo.astype(jnp.bfloat16), one, zero)
                    hot.append(jnp.concatenate([h, h], axis=0))
                got = jnp.dot(
                    field, jnp.concatenate(hot, axis=1), preferred_element_type=jnp.float32
                )
            for no, q in enumerate(pair):
                w = row8(sw, q, cols)
                here = [his[no] == t for t in range(tiles)]
                for r in range(frows // SUB):
                    sel = None
                    for t in range(tiles):
                        at = t * frows + r * SUB
                        if p < by_product:
                            taken = got[at : at + SUB, no * LANES : (no + 1) * LANES]
                        else:
                            taken = lanes_of(F[pl.ds(r * SUB, SUB), cols_of(b + t)], los[no])
                        sel = taken if t == 0 else jnp.where(here[t], taken, sel)
                    acc[r] = w * sel if acc[r] is None else acc[r] + w * sel
        for r in range(frows // SUB):
            U[pl.ds(r * SUB, SUB), cols] = acc[r]

    def upstreams(first, last):
        def both(i):
            upstream(first + 2 * i, False)
            upstream(first + 2 * i + 1, True)

        loop(0, (last - first) // 2, both)

    lane = lax.broadcasted_iota(jnp.int32, (SUB, LANES), 1)
    low_half = lane < NBR_REACH

    def around(ref, b, nvregs):
        before = jnp.maximum(b - 1, 0)
        after = jnp.minimum(b + 1, nb_blocks - 1)
        own_tiles, far_tiles = [], []
        for r in range(nvregs):
            rows = pl.ds(r * SUB, SUB)
            own_tiles.append(ref[rows, cols_of(b)])
            far_tiles.append(
                jnp.where(low_half, ref[rows, cols_of(after)], ref[rows, cols_of(before)])
            )
        return own_tiles, far_tiles

    def place(k, b, cols):
        x = row8(nb, k, cols)
        return x & (LANES - 1), (x >> (LANES.bit_length() - 1)) == b

    wrows = up8(2 * group)
    sub_iota = lax.broadcasted_iota(jnp.int32, (SUB, LANES), 0)

    def right_side(b):
        cols = cols_of(b)
        nv = wrows // SUB
        own_t, far_t = around(U, b, nv)
        acc = [jnp.zeros((SUB, LANES), jnp.float32)] * nv
        for k in range(sides):
            lo, here = place(k, b, cols)
            wx, wy = row8(gx, k, cols), row8(gy, k, cols)
            for r in range(nv):
                if (r + 1) * SUB <= group:
                    w = wx
                elif r * SUB >= group:
                    w = wy
                else:
                    w = jnp.where(sub_iota + r * SUB < group, wx, wy)
                taken = jnp.where(here, lanes_of(own_t[r], lo), lanes_of(far_t[r], lo))
                acc[r] = acc[r] + w * (taken - own_t[r])
        both = jnp.concatenate(acc, axis=0)
        div = both[0:group] + both[group : 2 * group]
        rx[lev, :, cols] = U[2 * group : 3 * group, cols] - COUPLING * div

    first = hb + REACH // LANES
    last = nb_blocks - first
    chunks = ((first + 1, last - 1), (0, first + 1), (last - 1, nb_blocks))

    def send(no):
        at = pl.ds(chunks[no][0] * LANES, (chunks[no][1] - chunks[no][0]) * LANES)
        started = []
        for d in range(1, nlev):
            copy = pltpu.make_async_remote_copy(
                src_ref=rx.at[lev, :, at],
                dst_ref=rx.at[lev, :, at],
                send_sem=lev_send.at[no, d - 1],
                recv_sem=lev_recv.at[no, d - 1],
                device_id={"lev": lax.rem(lev + d, nlev)},
                device_id_type=MESH,
            )
            copy.start()
            started.append(copy)
        return started

    def arrive(side):
        for copy in copies[side::2]:
            copy.wait_recv()
        at = slice(0, FIELD_HALO) if side == 0 else slice(FIELD_HALO + cells, 2 * FIELD_HALO + cells)
        for f in range(3):
            F[f * group : (f + 1) * group, at] = f_halo[side, f]
        at = slice(0, HALO) if side == 0 else slice(HALO + cells, ext)
        shift = -cells if side == 0 else cells
        si[:, at] = si_halo[side, :, 0, :] + (HALO + shift)
        sw[:, at] = sw_halo[side, :, 0, :]
        nb[:, at] = nb_halo[side] + (HALO - NBR_REACH + shift)
        lw[:, at] = lw_halo[side]
        gx[:, at] = ex_halo[side]
        gy[:, at] = ey_halo[side]

    upstreams(first, last)
    loop(*chunks[0], right_side, 2)
    sends = [send(0)]
    arrive(0)
    split_tiles(0, own_lo, G0)
    split_tiles(1, own_lo + 1, G1)
    upstreams(0, first)
    loop(*chunks[1], right_side, 7)
    sends.append(send(1))
    arrive(1)
    split_tiles(own_hi, ftiles, G0)
    split_tiles(own_hi - 1, ftiles, G1)
    upstreams(last, nb_blocks)
    loop(*chunks[2], right_side, 7)
    sends.append(send(2))
    for copy in copies:
        copy.wait_send()

    for f in range(2):
        winds[:, f, :] = U[f * group : (f + 1) * group, own]
    winds_copy = pltpu.make_async_copy(winds, winds_out, wind_sem)
    winds_copy.start()

    for copy in hc_copies:
        copy.wait()
    lrows = up8(levels)
    row = lax.broadcasted_iota(jnp.int32, (lrows, group), 0)
    col = lax.broadcasted_iota(jnp.int32, (lrows, group), 1)
    c = jnp.zeros((lrows, 1), jnp.float32)
    for g in range(nlev):
        c = c + jnp.sum(jnp.where(row - g * group == col, hc[g], 0.0), axis=1, keepdims=True)
    radius = 6.0 * c / (1.0 + 6.0 * c)
    steps = [
        jnp.broadcast_to(
            1.0 / (1.0 + radius * math.cos(math.pi * (2 * j + 1) / (2.0 * SWEEPS))), (lrows, LANES)
        )
        for j in range(SWEEPS)
    ]
    c = jnp.broadcast_to(c, (lrows, LANES))

    def modal(b):
        cols = cols_of(b)
        nv = lrows // SUB
        wsum = jnp.sum(lw[:, cols], axis=0, keepdims=True)
        total = [None] * nv
        for g in range(nlev):
            for i in range(group):
                x = jnp.broadcast_to(rx[g, pl.ds(i, 1), cols], (SUB, LANES))
                for r in range(nv):
                    term = to_wide[g * group + i, pl.ds(r * SUB, SUB)] * x
                    total[r] = term if total[r] is None else total[r] + term
        for r in range(nv):
            rows = pl.ds(r * SUB, SUB)
            cr = c[r * SUB : (r + 1) * SUB]
            inv = 1.0 / (1.0 + cr * wsum)
            scaled = total[r] * inv
            rinv[rows, cols] = scaled
            cinv[rows, cols] = cr * inv
            xa[rows, cols] = steps[0][r * SUB : (r + 1) * SUB] * scaled

    for no in range(len(chunks)):
        for copy in sends[no]:
            copy.wait_recv()
        loop(*chunks[no], modal, 2)

    x_old, x_new = xa, xb
    for j in range(1, SWEEPS):
        nv = lrows // SUB

        def sweep(b, x_old=x_old, x_new=x_new, j=j):
            cols = cols_of(b)
            own_t, far_t = around(x_old, b, nv)
            acc = [None] * nv
            for k in range(sides):
                lo, here = place(k, b, cols)
                w = row8(lw, k, cols)
                for r in range(nv):
                    term = w * jnp.where(here, lanes_of(own_t[r], lo), lanes_of(far_t[r], lo))
                    acc[r] = term if acc[r] is None else acc[r] + term
            for r in range(nv):
                rows = pl.ds(r * SUB, SUB)
                s = steps[j][r * SUB : (r + 1) * SUB]
                x_new[rows, cols] = (1.0 - s) * own_t[r] + s * (
                    rinv[rows, cols] + cinv[rows, cols] * acc[r]
                )

        margin = NBR_REACH * (SWEEPS - 1 - j)
        off = hb - -(-margin // LANES)
        loop(off, nb_blocks - off, sweep, 5)
        x_old, x_new = x_new, x_old

    def heights(b):
        nv = up8(group) // SUB
        cols = cols_of(b)
        total = [None] * nv
        for m in range(levels):
            x = jnp.broadcast_to(x_old[pl.ds(m, 1), cols_of(b + hb)], (SUB, LANES))
            for r in range(nv):
                term = from_wide[m, pl.ds(r * SUB, SUB)] * x
                total[r] = term if total[r] is None else total[r] + term
        height_out[:, cols] = jnp.concatenate(total, axis=0)[0:group]

    loop(0, cells // LANES, heights, 2)
    winds_copy.wait()
    for started in sends:
        for copy in started:
            copy.wait_send()


def per_device(npatch, nlev, *args):
    fields, s_index, _, nbr = args[:4]
    _, group, cells = fields.shape
    points, sides = s_index.shape[0], nbr.shape[0]
    levels = group * nlev
    ext = cells + 2 * HALO
    f32, i32 = jnp.float32, jnp.int32
    args = args[:-1] + (args[-1].reshape(1, group),)
    lrows = up8(levels)
    vm = pltpu.VMEM
    peers = max(nlev - 1, 1)
    winds, height = pl.pallas_call(
        functools.partial(kernel, npatch, nlev),
        out_shape=(
            jax.ShapeDtypeStruct((group, 2, cells), f32),
            jax.ShapeDtypeStruct((group, cells), f32),
        ),
        in_specs=[pl.BlockSpec(memory_space=pl.ANY)] * 7
        + [pl.BlockSpec(memory_space=pltpu.VMEM)] * 3,
        out_specs=(
            pl.BlockSpec(memory_space=pl.ANY),
            pl.BlockSpec(memory_space=pltpu.VMEM),
        ),
        scratch_shapes=[vm(a.shape, a.dtype) for a in args[:7]]
        + [
            vm((group, 2, cells), f32),
            pltpu.SemaphoreType.DMA((7,)),
            pltpu.SemaphoreType.DMA,
            vm((2, 3, group, FIELD_HALO), f32),
            vm((2, points, 1, HALO), i32),
            vm((2, points, 1, HALO), f32),
            vm((2, sides, HALO), i32),
            vm((2, sides, HALO), f32),
            vm((2, sides, HALO), f32),
            vm((2, sides, HALO), f32),
            vm((nlev, 1, group), f32),
            vm((up8(3 * group), cells + 2 * FIELD_HALO), f32),
            vm((up8(3 * group) * ((cells + 2 * FIELD_HALO) // LANES + 2), 2 * LANES), jnp.bfloat16),
            vm((up8(3 * group) * ((cells + 2 * FIELD_HALO) // LANES + 2), 2 * LANES), jnp.bfloat16),
            vm((points, ext), i32),
            vm((points, ext), f32),
            vm((sides, ext), i32),
            vm((sides, ext), f32),
            vm((sides, ext), f32),
            vm((sides, ext), f32),
            vm((up8(3 * group), ext), f32),
            vm((nlev, group, ext), f32),
            vm((lrows, ext), f32),
            vm((lrows, ext), f32),
            vm((lrows, ext), f32),
            vm((lrows, ext), f32),
            vm((levels, lrows, LANES), f32),
            vm((levels, up8(group), LANES), f32),
            pltpu.SemaphoreType.DMA((14,)),
            pltpu.SemaphoreType.DMA((14,)),
            pltpu.SemaphoreType.DMA((3, peers)),
            pltpu.SemaphoreType.DMA((3, peers)),
            pltpu.SemaphoreType.DMA((peers,)),
            pltpu.SemaphoreType.DMA((peers,)),
        ],
        compiler_params=pltpu.CompilerParams(
            collective_id=0, has_side_effects=True
        ),
    )(*args)
    return jnp.transpose(winds, (1, 0, 2)), height


def solution(mesh):
    in_specs = (
        P(None, "lev", "patch"),
        P(None, "lev", "patch"),
        P(None, "lev", "patch"),
        P(None, "patch"),
        P(None, "patch"),
        P(None, "patch"),
        P(None, "patch"),
        P(),
        P(),
        P("lev"),
    )
    out_specs = (P(None, "lev", "patch"), P("lev", "patch"))
    body = functools.partial(per_device, mesh.shape["patch"], mesh.shape["lev"])
    return jax.shard_map(
        body, mesh=mesh, in_specs=in_specs, out_specs=out_specs, check_vma=False
    )
```

```python
import functools
import math

import jax
import jax.numpy as jnp
from jax import lax
from jax.experimental import pallas as pl
from jax.experimental.pallas import tpu as pltpu
from jax.sharding import PartitionSpec as P

REACH = 512
NBR_REACH = 64
SWEEPS = 4
COUPLING = 0.5
LANES = 128
SUB = 8
HALO = NBR_REACH * SWEEPS
FIELD_HALO = REACH + HALO
MESH = pl.DeviceIdType.MESH


BITS = LANES.bit_length() - 1
bf16, f32, i32 = jnp.bfloat16, jnp.float32, jnp.int32


def up8(rows):
    return -(-rows // SUB) * SUB


def split(x):
    high = x.astype(bf16)
    return high, (x - high.astype(f32)).astype(bf16)


def product(parts, x):
    high, low = split(x)
    dot = functools.partial(jnp.dot, preferred_element_type=f32)
    return dot(parts[0], high) + (dot(parts[1], high) + dot(parts[0], low))


def lanes_of(x, index):
    return jnp.take_along_axis(x, index, axis=1, mode="promise_in_bounds")


def row8(ref, row, cols):
    return jnp.broadcast_to(ref[pl.ds(row, 1), cols], (SUB, LANES))


def cols_of(block):
    if isinstance(block, int):
        return slice(block * LANES, (block + 1) * LANES)
    return pl.ds(pl.multiple_of(block * LANES, LANES), LANES)


def loop(first, count, body, unroll=1):
    trips = count // unroll

    def step(i, carry):
        for u in range(unroll):
            body(first + i * unroll + u)
        return carry

    if trips == 1:
        step(0, 0)
    else:
        lax.fori_loop(0, trips, step, 0)
    for u in range(trips * unroll, count):
        body(first + u)


def kernel(
    npatch, nlev,
    fields_in, s_index_in, s_weight_in, nbr_in, lap_in, ex_in, ey_in, to_modes, from_modes, helm,
    winds_out, height_out,
    fields, s_index, s_weight, nbr, lap, ex, ey, winds, load_sem, wind_sem,
    f_halo, si_halo, sw_halo, nb_halo, lw_halo, ex_halo, ey_halo, hc,
    F, G0, G1, si, sw, nb, lw, gx, gy, U, rx, rinv, cinv, xa, xb,
    send_sem, recv_sem, lev_send, lev_recv, hc_send, hc_recv,
):
    group = fields.shape[1]
    cells = fields.shape[2]
    levels = group * nlev
    points = s_index.shape[0]
    sides = nbr.shape[0]
    ext = cells + 2 * HALO
    nb_blocks = ext // LANES
    own_blocks = cells // LANES
    hb = HALO // LANES
    patch = lax.axis_index("patch")
    lev = lax.axis_index("lev")
    right = lax.rem(patch + 1, npatch)
    left = lax.rem(patch + npatch - 1, npatch)

    barrier = pltpu.get_barrier_semaphore()
    for to in (left, right):
        pl.semaphore_signal(barrier, inc=1, device_id={"patch": to}, device_id_type=MESH)
    for d in range(1, nlev):
        pl.semaphore_signal(
            barrier, inc=1, device_id={"lev": lax.rem(lev + d, nlev)}, device_id_type=MESH
        )
    loads = []
    for no, (src, dst) in enumerate((
        (fields_in, fields), (s_index_in, s_index), (s_weight_in, s_weight),
        (nbr_in, nbr), (lap_in, lap), (ex_in, ex), (ey_in, ey),
    )):
        copy = pltpu.make_async_copy(src, dst, load_sem.at[no])
        copy.start()
        loads.append(copy)
    hc[lev] = helm[...]

    pairs = (
        (s_index_in, si_halo, HALO),
        (s_weight_in, sw_halo, HALO),
        (fields_in, f_halo, FIELD_HALO),
        (nbr_in, nb_halo, HALO),
        (ex_in, ex_halo, HALO),
        (ey_in, ey_halo, HALO),
        (lap_in, lw_halo, HALO),
    )

    def halo_copies(side):
        made = []
        for no, (src, dst, width) in enumerate(pairs):
            lead = (slice(None),) * (len(src.shape) - 1)
            start = (1 - side) * (cells - width)
            if not isinstance(side, int):
                start = pl.multiple_of(start, LANES)
            made.append(pltpu.make_async_remote_copy(
                src_ref=src.at[lead + (pl.ds(start, width),)],
                dst_ref=dst.at[side],
                send_sem=send_sem.at[2 * no + side],
                recv_sem=recv_sem.at[2 * no + side],
                device_id={"patch": lax.rem(patch + npatch + 1 - 2 * side, npatch)},
                device_id_type=MESH,
            ))
        return made

    def helm_copies():
        return [
            pltpu.make_async_remote_copy(
                src_ref=helm,
                dst_ref=hc.at[lev],
                send_sem=hc_send.at[d - 1],
                recv_sem=hc_recv.at[d - 1],
                device_id={"lev": lax.rem(lev + d, nlev)},
                device_id_type=MESH,
            )
            for d in range(1, nlev)
        ]

    def meet_and_send():
        pl.semaphore_wait(barrier, 2 + nlev - 1)
        for side in (0, 1):
            for copy in halo_copies(side):
                copy.start()
        for copy in helm_copies():
            copy.start()

    @pl.when(patch != 0)
    def _():
        meet_and_send()

    frows = F.shape[0]
    tiles = 2 * REACH // LANES + 1
    ftiles = F.shape[1] // LANES
    own_lo = FIELD_HALO // LANES
    own_hi = own_lo + own_blocks

    def split_pair(tile, odd, to):
        start = tile * frows + (frows if odd else 0) % (2 * SUB)
        if not isinstance(tile, int):
            start = pl.multiple_of(start, 2 * SUB)
        rows = pl.ds(start, 2 * frows)
        high, low = split(
            jnp.concatenate([F[:, cols_of(tile)], F[:, cols_of(tile + 1)]], axis=0)
        )
        to[rows, 0:LANES] = high
        to[rows, LANES : 2 * LANES] = low

    lane_id = lax.broadcasted_iota(i32, (LANES, LANES), 0).astype(f32).astype(bf16)
    one = jnp.ones((LANES, LANES), bf16)
    zero = jnp.zeros((LANES, LANES), bf16)

    def upstream(b, odd, by_lane=(2, 5)):
        cols = cols_of(b)
        nv = frows // SUB
        acc = [None] * nv
        start = b * frows + (frows if odd else 0) % (2 * SUB)
        if not isinstance(b, int):
            start = pl.multiple_of(start, 2 * SUB)
        field = (G1 if odd else G0).at[pl.ds(start, tiles * frows), :]
        for pair_no in range(points // 2):
            pair = (2 * pair_no, 2 * pair_no + 1)
            his, los = [], []
            for q in pair:
                x = row8(si, q, cols)
                his.append((x >> BITS) - b)
                los.append(x & (LANES - 1))
            on_lanes = pair_no in by_lane
            if not on_lanes:
                hot = []
                for lo in los:
                    lo = jnp.broadcast_to(lo[0:1].astype(f32), (LANES, LANES))
                    h = jnp.where(lane_id == lo.astype(bf16), one, zero)
                    hot.append(jnp.concatenate([h, h], axis=0))
                got = jnp.dot(
                    field[...], jnp.concatenate(hot, axis=1), preferred_element_type=f32
                )
            for no, q in enumerate(pair):
                w = row8(sw, q, cols)
                here = [his[no] == t for t in range(tiles)]
                for r in range(nv):
                    sel = None
                    for t in range(tiles):
                        row = t * frows + r * SUB
                        if on_lanes:
                            taken = lanes_of(
                                F[r * SUB : (r + 1) * SUB, cols_of(b + t)], los[no]
                            )
                        else:
                            taken = got[row : row + SUB, no * LANES : (no + 1) * LANES]
                        sel = taken if sel is None else jnp.where(here[t], taken, sel)
                    acc[r] = w * sel if acc[r] is None else acc[r] + w * sel
        for r in range(nv):
            U[r * SUB : (r + 1) * SUB, cols] = acc[r]

    lane = lax.broadcasted_iota(i32, (SUB, LANES), 1)
    low_half = lane < NBR_REACH

    def around(ref, b, nvregs):
        before = jnp.maximum(b - 1, 0)
        after = jnp.minimum(b + 1, nb_blocks - 1)
        own_tiles, far_tiles = [], []
        for r in range(nvregs):
            rows = pl.ds(r * SUB, SUB)
            own_tiles.append(ref[rows, cols_of(b)])
            far_tiles.append(
                jnp.where(low_half, ref[rows, cols_of(after)], ref[rows, cols_of(before)])
            )
        return own_tiles, far_tiles

    def place(k, b, cols):
        x = row8(nb, k, cols)
        return x & (LANES - 1), (x >> BITS) == b

    wrows = up8(2 * group)
    sub_iota = lax.broadcasted_iota(i32, (SUB, LANES), 0)

    def right_side(b):
        cols = cols_of(b)
        nv = wrows // SUB
        own_t, far_t = around(U, b, nv)
        acc = [jnp.zeros((SUB, LANES), f32)] * nv
        for k in range(sides):
            lo, here = place(k, b, cols)
            wx, wy = row8(gx, k, cols), row8(gy, k, cols)
            for r in range(nv):
                if (r + 1) * SUB <= group:
                    w = wx
                elif r * SUB >= group:
                    w = wy
                else:
                    w = jnp.where(sub_iota + r * SUB < group, wx, wy)
                taken = jnp.where(here, lanes_of(own_t[r], lo), lanes_of(far_t[r], lo))
                acc[r] = acc[r] + w * (taken - own_t[r])
        both = jnp.concatenate(acc, axis=0)
        div = both[0:group] + both[group : 2 * group]
        rx[lev, :, cols] = U[2 * group : 3 * group, cols] - COUPLING * div

    first = hb + REACH // LANES
    last = nb_blocks - first
    inner = (first + 1, last - first - 2)
    outer = first + 1

    def lev_copies(no, at, count):
        at = pl.ds(at * LANES if isinstance(at, int) else pl.multiple_of(at * LANES, LANES), count * LANES)
        return [
            pltpu.make_async_remote_copy(
                src_ref=rx.at[lev, :, at],
                dst_ref=rx.at[lev, :, at],
                send_sem=lev_send.at[no, d - 1],
                recv_sem=lev_recv.at[no, d - 1],
                device_id={"lev": lax.rem(lev + d, nlev)},
                device_id_type=MESH,
            )
            for d in range(1, nlev)
        ]

    def arrive(side):
        for copy in halo_copies(side):
            copy.wait_recv()
        at = pl.ds(pl.multiple_of(side * (FIELD_HALO + cells), LANES), FIELD_HALO)
        for f in range(3):
            F[f * group : (f + 1) * group, at] = f_halo[side, f]
        for i in range(0, own_lo, 2):
            split_pair(side * own_hi + i, False, G0)
        for i in range(1, own_lo + 2, 2):
            split_pair(side * (own_hi - 2) + i, True, G1)
        at = pl.ds(pl.multiple_of(side * (HALO + cells), LANES), HALO)
        shift = HALO + (2 * side - 1) * cells
        si[:, at] = si_halo[side, :, 0, :] + shift
        sw[:, at] = sw_halo[side, :, 0, :]
        nb[:, at] = nb_halo[side] + (shift - NBR_REACH)
        lw[:, at] = lw_halo[side]
        gx[:, at] = ex_halo[side]
        gy[:, at] = ey_halo[side]

    for copy in loads:
        copy.wait()
    for f in range(3):
        F[f * group : (f + 1) * group, FIELD_HALO : FIELD_HALO + cells] = fields[f]
    own = slice(HALO, HALO + cells)
    si[:, own] = s_index[:, 0, :] + HALO
    sw[:, own] = s_weight[:, 0, :]
    for tile in range(own_lo, own_hi, 2):
        split_pair(tile, False, G0)
    for tile in range(own_lo + 1, own_hi, 2):
        split_pair(tile, True, G1)
    for b in range(first, last):
        upstream(b, b % 2)
    nb[:, own] = nbr[...] + (HALO - NBR_REACH)
    lw[:, own] = lap[...]
    gx[:, own] = ex[...]
    gy[:, own] = ey[...]

    @pl.when(patch == 0)
    def _():
        meet_and_send()

    loop(*inner, right_side, inner[1])
    for copy in lev_copies(0, *inner):
        copy.start()
    begin = jnp.where(patch == 1, 1, 1 - lax.rem(patch, 2))

    def flank(turn, carry):
        side = begin + turn * (1 - 2 * begin)
        arrive(side)
        for i in range(first):
            upstream(side * last + i, i % 2)
        loop(side * (last - 1), outer, right_side, outer)
        for copy in lev_copies(1 + turn, side * (last - 1), outer):
            copy.start()
        return carry

    lax.fori_loop(0, 2, flank, 0)

    for f in range(2):
        winds[:, f, :] = U[f * group : (f + 1) * group, own]
    winds_copy = pltpu.make_async_copy(winds, winds_out, wind_sem)
    winds_copy.start()

    for copy in helm_copies():
        copy.wait()
    lrows = up8(levels)
    row = lax.broadcasted_iota(i32, (lrows, group), 0)
    col = lax.broadcasted_iota(i32, (lrows, group), 1)
    c = jnp.zeros((lrows, 1), f32)
    for g in range(nlev):
        c = c + jnp.sum(jnp.where(row - g * group == col, hc[g], 0.0), axis=1, keepdims=True)
    radius = 6.0 * c / (1.0 + 6.0 * c)
    steps = [
        jnp.broadcast_to(
            1.0 / (1.0 + radius * math.cos(math.pi * (2 * j + 1) / (2.0 * SWEEPS))), (lrows, LANES)
        )
        for j in range(SWEEPS)
    ]
    c = jnp.broadcast_to(c, (lrows, LANES))
    nv = lrows // SUB
    to_parts = split(to_modes[...])
    back = from_modes[0:group, :]
    for g in range(1, nlev):
        back = jnp.where(lev == g, from_modes[g * group : (g + 1) * group, :], back)
    back_parts = split(back)

    def modal(b):
        cols = cols_of(b)
        wsum = jnp.sum(lw[:, cols], axis=0, keepdims=True)
        total = product(to_parts, jnp.concatenate([rx[g, :, cols] for g in range(nlev)], axis=0))
        for r in range(nv):
            rows = pl.ds(r * SUB, SUB)
            cr = c[r * SUB : (r + 1) * SUB]
            inv = 1.0 / (1.0 + cr * wsum)
            scaled = total[r * SUB : (r + 1) * SUB] * inv
            rinv[rows, cols] = scaled
            cinv[rows, cols] = cr * inv
            xa[rows, cols] = steps[0][r * SUB : (r + 1) * SUB] * scaled

    def sweep(j, b):
        x_old, x_new = (xa, xb) if j % 2 else (xb, xa)
        cols = cols_of(b)
        own_t, far_t = around(x_old, b, nv)
        acc = [None] * nv
        for k in range(sides):
            lo, here = place(k, b, cols)
            w = row8(lw, k, cols)
            for r in range(nv):
                term = w * jnp.where(here, lanes_of(own_t[r], lo), lanes_of(far_t[r], lo))
                acc[r] = term if acc[r] is None else acc[r] + term
        for r in range(nv):
            rows = pl.ds(r * SUB, SUB)
            s = steps[j][r * SUB : (r + 1) * SUB]
            x_new[rows, cols] = (1.0 - s) * own_t[r] + s * (
                rinv[rows, cols] + cinv[rows, cols] * acc[r]
            )

    x_end = xa if SWEEPS % 2 else xb

    def heights(b):
        height_out[:, cols_of(b - hb)] = product(back_parts, x_end[0:levels, cols_of(b)])

    def off(j):
        return hb - -(-(NBR_REACH * (SWEEPS - 1 - j)) // LANES)

    def finish(side, first_part):
        def part(at, j):
            width = nb_blocks - outer if first_part else outer
            low = (nb_blocks - width) * side
            if j == 0:
                return low, width
            grow = -j if first_part else j
            width = width + grow - at
            return low + jnp.where(side == 0, at, -grow), width

        many = 1 if nv > 4 else nb_blocks
        loop(*part(0, 0), modal, min(many, part(0, 0)[1]))
        for j in range(1, SWEEPS):
            start, count = part(off(j), j)
            loop(start, count, functools.partial(sweep, j), min(many, count))
        start, count = part(hb, SWEEPS - 1)
        loop(start, count, heights, count)

    for copy in lev_copies(0, *inner) + lev_copies(1, begin * (last - 1), outer):
        copy.wait_recv()
    finish(begin, True)
    for copy in lev_copies(2, (1 - begin) * (last - 1), outer):
        copy.wait_recv()
    finish(1 - begin, False)
    winds_copy.wait()
    for side in (0, 1):
        for copy in halo_copies(side):
            copy.wait_send()
    for copy in lev_copies(0, *inner):
        copy.wait_send()
    for no in (1, 2):
        for copy in lev_copies(no, 0, outer):
            copy.wait_send()


def per_device(npatch, nlev, *args):
    fields, s_index, _, nbr = args[:4]
    _, group, cells = fields.shape
    points, sides = s_index.shape[0], nbr.shape[0]
    levels = group * nlev
    ext = cells + 2 * HALO
    args = args[:-1] + (args[-1].reshape(1, group),)
    lrows = up8(levels)
    vm = pltpu.VMEM
    peers = max(nlev - 1, 1)
    winds, height = pl.pallas_call(
        functools.partial(kernel, npatch, nlev),
        out_shape=(
            jax.ShapeDtypeStruct((group, 2, cells), f32),
            jax.ShapeDtypeStruct((group, cells), f32),
        ),
        in_specs=[pl.BlockSpec(memory_space=pl.ANY)] * 7
        + [pl.BlockSpec(memory_space=pltpu.VMEM)] * 3,
        out_specs=(
            pl.BlockSpec(memory_space=pl.ANY),
            pl.BlockSpec(memory_space=pltpu.VMEM),
        ),
        scratch_shapes=[vm(a.shape, a.dtype) for a in args[:7]]
        + [
            vm((group, 2, cells), f32),
            pltpu.SemaphoreType.DMA((7,)),
            pltpu.SemaphoreType.DMA,
            vm((2, 3, group, FIELD_HALO), f32),
            vm((2, points, 1, HALO), i32),
            vm((2, points, 1, HALO), f32),
            vm((2, sides, HALO), i32),
            vm((2, sides, HALO), f32),
            vm((2, sides, HALO), f32),
            vm((2, sides, HALO), f32),
            vm((nlev, 1, group), f32),
            vm((up8(3 * group), cells + 2 * FIELD_HALO + LANES), f32),
            vm((up8(3 * group) * ((cells + 2 * FIELD_HALO) // LANES + 2), 2 * LANES), bf16),
            vm((up8(3 * group) * ((cells + 2 * FIELD_HALO) // LANES + 2), 2 * LANES), bf16),
            vm((points, ext), i32),
            vm((points, ext), f32),
            vm((sides, ext), i32),
            vm((sides, ext), f32),
            vm((sides, ext), f32),
            vm((sides, ext), f32),
            vm((up8(3 * group), ext), f32),
            vm((nlev, group, ext), f32),
            vm((lrows, ext), f32),
            vm((lrows, ext), f32),
            vm((lrows, ext), f32),
            vm((lrows, ext), f32),
            pltpu.SemaphoreType.DMA((14,)),
            pltpu.SemaphoreType.DMA((14,)),
            pltpu.SemaphoreType.DMA((3, peers)),
            pltpu.SemaphoreType.DMA((3, peers)),
            pltpu.SemaphoreType.DMA((peers,)),
            pltpu.SemaphoreType.DMA((peers,)),
        ],
        compiler_params=pltpu.CompilerParams(
            collective_id=0, has_side_effects=True
        ),
    )(*args)
    return jnp.transpose(winds, (1, 0, 2)), height


def solution(mesh):
    in_specs = (
        P(None, "lev", "patch"),
        P(None, "lev", "patch"),
        P(None, "lev", "patch"),
        P(None, "patch"),
        P(None, "patch"),
        P(None, "patch"),
        P(None, "patch"),
        P(),
        P(),
        P("lev"),
    )
    out_specs = (P(None, "lev", "patch"), P("lev", "patch"))
    body = functools.partial(per_device, mesh.shape["patch"], mesh.shape["lev"])
    return jax.shard_map(
        body, mesh=mesh, in_specs=in_specs, out_specs=out_specs, check_vma=False
    )
```

```python
import functools
import math

import jax
import jax.numpy as jnp
from jax import lax
from jax.experimental import pallas as pl
from jax.experimental.pallas import tpu as pltpu
from jax.sharding import PartitionSpec as P

REACH = 512
NBR_REACH = 64
SWEEPS = 4
COUPLING = 0.5
LANES = 128
SUB = 8
HALO = NBR_REACH * SWEEPS
FIELD_HALO = REACH + HALO
MESH = pl.DeviceIdType.MESH


BITS = LANES.bit_length() - 1
bf16, f32, i32 = jnp.bfloat16, jnp.float32, jnp.int32


def up8(rows):
    return -(-rows // SUB) * SUB


def split(x):
    high = x.astype(bf16)
    return high, (x - high.astype(f32)).astype(bf16)


def product(parts, x):
    high, low = split(x)
    dot = functools.partial(jnp.dot, preferred_element_type=f32)
    return dot(parts[0], high) + (dot(parts[1], high) + dot(parts[0], low))


def lanes_of(x, index):
    return jnp.take_along_axis(x, index, axis=1, mode="promise_in_bounds")


def row8(ref, row, cols):
    return jnp.broadcast_to(ref[pl.ds(row, 1), cols], (SUB, LANES))


def cols_of(block):
    if isinstance(block, int):
        return slice(block * LANES, (block + 1) * LANES)
    return pl.ds(pl.multiple_of(block * LANES, LANES), LANES)


def loop(first, count, body, unroll=1):
    trips = count // unroll

    def step(i, carry):
        for u in range(unroll):
            body(first + i * unroll + u)
        return carry

    if trips == 1:
        step(0, 0)
    else:
        lax.fori_loop(0, trips, step, 0)
    for u in range(trips * unroll, count):
        body(first + u)


def kernel(
    npatch, nlev,
    fields_in, s_index_in, s_weight_in, nbr_in, lap_in, ex_in, ey_in, to_modes, from_modes, helm,
    winds_out, height_out,
    fields, s_index, s_weight, nbr, lap, ex, ey, load_sem,
    f_halo, si_halo, sw_halo, nb_halo, lw_halo, ex_halo, ey_halo, hc,
    F, G0, G1, si, sw, nb, lw, gx, gy, U, rx, rinv, cinv, xa, xb,
    near_sem, send_sem, recv_sem, lev_send, lev_recv, hc_send, hc_recv,
):
    group = fields.shape[1]
    cells = fields.shape[2]
    levels = group * nlev
    points = s_index.shape[0]
    sides = nbr.shape[0]
    ext = cells + 2 * HALO
    nb_blocks = ext // LANES
    own_blocks = cells // LANES
    hb = HALO // LANES
    patch = lax.axis_index("patch")
    lev = lax.axis_index("lev")
    right = lax.rem(patch + 1, npatch)
    left = lax.rem(patch + npatch - 1, npatch)

    barrier = pltpu.get_barrier_semaphore()
    pl.semaphore_signal(barrier, inc=1, device_id={"patch": right}, device_id_type=MESH)

    @pl.when(patch != 1)
    def _():
        pl.semaphore_signal(barrier, inc=1, device_id={"patch": left}, device_id_type=MESH)

    for d in range(1, nlev):
        pl.semaphore_signal(
            barrier, inc=1, device_id={"lev": lax.rem(lev + d, nlev)}, device_id_type=MESH
        )
    loads = []
    for no, (src, dst) in enumerate((
        (fields_in, fields), (s_index_in, s_index), (s_weight_in, s_weight),
        (nbr_in, nbr), (lap_in, lap), (ex_in, ex), (ey_in, ey),
    )):
        copy = pltpu.make_async_copy(src, dst, load_sem.at[no])
        copy.start()
        loads.append(copy)
    hc[lev] = helm[...]

    pairs = (
        (s_index_in, si_halo, HALO),
        (s_weight_in, sw_halo, HALO),
        (fields_in, f_halo, FIELD_HALO),
        (nbr_in, nb_halo, HALO),
        (ex_in, ex_halo, HALO),
        (ey_in, ey_halo, HALO),
        (lap_in, lw_halo, HALO),
    )

    def halo_copies(side):
        made = []
        for no, (src, dst, width) in enumerate(pairs):
            lead = (slice(None),) * (len(src.shape) - 1)
            start = (1 - side) * (cells - width)
            if not isinstance(side, int):
                start = pl.multiple_of(start, LANES)
            made.append(pltpu.make_async_remote_copy(
                src_ref=src.at[lead + (pl.ds(start, width),)],
                dst_ref=dst.at[side],
                send_sem=send_sem.at[2 * no + side],
                recv_sem=recv_sem.at[2 * no + side],
                device_id={"patch": lax.rem(patch + npatch + 1 - 2 * side, npatch)},
                device_id_type=MESH,
            ))
        return made

    def helm_copies():
        return [
            pltpu.make_async_remote_copy(
                src_ref=helm,
                dst_ref=hc.at[lev],
                send_sem=hc_send.at[d - 1],
                recv_sem=hc_recv.at[d - 1],
                device_id={"lev": lax.rem(lev + d, nlev)},
                device_id_type=MESH,
            )
            for d in range(1, nlev)
        ]

    def start(made):
        for copy in made:
            copy.start()

    @pl.when(patch != 0)
    def _():
        pl.semaphore_wait(barrier, 2 + nlev - 1)

    @pl.when(patch == 1)
    def _():
        pl.semaphore_signal(near_sem, inc=1, device_id={"patch": left}, device_id_type=MESH)

    @pl.when(patch != 0)
    def _():
        start(halo_copies(0) + halo_copies(1) + helm_copies())

    frows = F.shape[0]
    tiles = 2 * REACH // LANES + 1
    ftiles = F.shape[1] // LANES
    own_lo = FIELD_HALO // LANES
    own_hi = own_lo + own_blocks

    def split_pair(tile, odd, to):
        start = tile * frows + (frows if odd else 0) % (2 * SUB)
        if not isinstance(tile, int):
            start = pl.multiple_of(start, 2 * SUB)
        rows = pl.ds(start, 2 * frows)
        high, low = split(
            jnp.concatenate([F[:, cols_of(tile)], F[:, cols_of(tile + 1)]], axis=0)
        )
        to[rows, 0:LANES] = high
        to[rows, LANES : 2 * LANES] = low

    lane_id = lax.broadcasted_iota(i32, (LANES, LANES), 0).astype(f32).astype(bf16)
    one = jnp.ones((LANES, LANES), bf16)
    zero = jnp.zeros((LANES, LANES), bf16)

    def upstream(b, odd, by_lane=(2, 5)):
        cols = cols_of(b)
        nv = frows // SUB
        acc = [None] * nv
        start = b * frows + (frows if odd else 0) % (2 * SUB)
        if not isinstance(b, int):
            start = pl.multiple_of(start, 2 * SUB)
        field = (G1 if odd else G0).at[pl.ds(start, tiles * frows), :]
        for pair_no in range(points // 2):
            pair = (2 * pair_no, 2 * pair_no + 1)
            his, los = [], []
            for q in pair:
                x = row8(si, q, cols)
                his.append((x >> BITS) - b)
                los.append(x & (LANES - 1))
            on_lanes = pair_no in by_lane
            if not on_lanes:
                hot = []
                for lo in los:
                    lo = jnp.broadcast_to(lo[0:1].astype(f32), (LANES, LANES))
                    h = jnp.where(lane_id == lo.astype(bf16), one, zero)
                    hot.append(jnp.concatenate([h, h], axis=0))
                got = jnp.dot(
                    field[...], jnp.concatenate(hot, axis=1), preferred_element_type=f32
                )
            for no, q in enumerate(pair):
                w = row8(sw, q, cols)
                here = [his[no] == t for t in range(tiles)]
                for r in range(nv):
                    sel = None
                    for t in range(tiles):
                        row = t * frows + r * SUB
                        if on_lanes:
                            taken = lanes_of(
                                F[r * SUB : (r + 1) * SUB, cols_of(b + t)], los[no]
                            )
                        else:
                            taken = got[row : row + SUB, no * LANES : (no + 1) * LANES]
                        sel = taken if sel is None else jnp.where(here[t], taken, sel)
                    acc[r] = w * sel if acc[r] is None else acc[r] + w * sel
        for r in range(nv):
            U[r * SUB : (r + 1) * SUB, cols] = acc[r]

    lane = lax.broadcasted_iota(i32, (SUB, LANES), 1)
    low_half = lane < NBR_REACH

    def around(ref, b, nvregs):
        before = jnp.maximum(b - 1, 0)
        after = jnp.minimum(b + 1, nb_blocks - 1)
        own_tiles, far_tiles = [], []
        for r in range(nvregs):
            rows = pl.ds(r * SUB, SUB)
            own_tiles.append(ref[rows, cols_of(b)])
            far_tiles.append(
                jnp.where(low_half, ref[rows, cols_of(after)], ref[rows, cols_of(before)])
            )
        return own_tiles, far_tiles

    def place(k, b, cols):
        x = row8(nb, k, cols)
        return x & (LANES - 1), (x >> BITS) == b

    wrows = up8(2 * group)
    sub_iota = lax.broadcasted_iota(i32, (SUB, LANES), 0)

    def right_side(b):
        cols = cols_of(b)
        nv = wrows // SUB
        own_t, far_t = around(U, b, nv)
        acc = [jnp.zeros((SUB, LANES), f32)] * nv
        for k in range(sides):
            lo, here = place(k, b, cols)
            wx, wy = row8(gx, k, cols), row8(gy, k, cols)
            for r in range(nv):
                if (r + 1) * SUB <= group:
                    w = wx
                elif r * SUB >= group:
                    w = wy
                else:
                    w = jnp.where(sub_iota + r * SUB < group, wx, wy)
                taken = jnp.where(here, lanes_of(own_t[r], lo), lanes_of(far_t[r], lo))
                acc[r] = acc[r] + w * (taken - own_t[r])
        both = jnp.concatenate(acc, axis=0)
        div = both[0:group] + both[group : 2 * group]
        rx[lev, :, cols] = U[2 * group : 3 * group, cols] - COUPLING * div

    first = hb + REACH // LANES
    last = nb_blocks - first
    inner = (first + 1, last - first - 2)
    outer = first + 1

    def lev_copies(no, at, count):
        at = pl.ds(at * LANES if isinstance(at, int) else pl.multiple_of(at * LANES, LANES), count * LANES)
        return [
            pltpu.make_async_remote_copy(
                src_ref=rx.at[lev, :, at],
                dst_ref=rx.at[lev, :, at],
                send_sem=lev_send.at[no, d - 1],
                recv_sem=lev_recv.at[no, d - 1],
                device_id={"lev": lax.rem(lev + d, nlev)},
                device_id_type=MESH,
            )
            for d in range(1, nlev)
        ]

    def arrive(side):
        for copy in halo_copies(side):
            copy.wait_recv()
        at = pl.ds(pl.multiple_of(side * (FIELD_HALO + cells), LANES), FIELD_HALO)
        for f in range(3):
            F[f * group : (f + 1) * group, at] = f_halo[side, f]
        for i in range(0, own_lo, 2):
            split_pair(side * own_hi + i, False, G0)
        for i in range(1, own_lo + 2, 2):
            split_pair(side * (own_hi - 2) + i, True, G1)
        at = pl.ds(pl.multiple_of(side * (HALO + cells), LANES), HALO)
        shift = HALO + (2 * side - 1) * cells
        si[:, at] = si_halo[side, :, 0, :] + shift
        sw[:, at] = sw_halo[side, :, 0, :]
        nb[:, at] = nb_halo[side] + (shift - NBR_REACH)
        lw[:, at] = lw_halo[side]
        gx[:, at] = ex_halo[side]
        gy[:, at] = ey_halo[side]

    for copy in loads:
        copy.wait()
    for f in range(3):
        F[f * group : (f + 1) * group, FIELD_HALO : FIELD_HALO + cells] = fields[f]
    own = slice(HALO, HALO + cells)
    si[:, own] = s_index[:, 0, :] + HALO
    sw[:, own] = s_weight[:, 0, :]
    for tile in range(own_lo, own_hi, 2):
        split_pair(tile, False, G0)
    for tile in range(own_lo + 1, own_hi, 2):
        split_pair(tile, True, G1)
    middle = first + 2
    for b in range(first, middle):
        upstream(b, b % 2)

    @pl.when(patch == 0)
    def _():
        pl.semaphore_wait(near_sem, 1)
        start(halo_copies(0))

    for b in range(middle, last):
        upstream(b, b % 2)
    nb[:, own] = nbr[...] + (HALO - NBR_REACH)
    lw[:, own] = lap[...]
    gx[:, own] = ex[...]
    gy[:, own] = ey[...]

    @pl.when(patch == 0)
    def _():
        pl.semaphore_wait(barrier, 2 + nlev - 2)
        start(halo_copies(1) + helm_copies())

    loop(*inner, right_side, inner[1])
    for copy in lev_copies(0, *inner):
        copy.start()
    begin = 1 - lax.rem(patch, 2)

    def flank(turn, carry):
        side = begin + turn * (1 - 2 * begin)
        arrive(side)
        for i in range(first):
            upstream(side * last + i, i % 2)
        loop(side * (last - 1), outer, right_side, outer)
        for copy in lev_copies(1 + turn, side * (last - 1), outer):
            copy.start()
        return carry

    lax.fori_loop(0, 2, flank, 0)

    for f in range(2):
        winds_out[:, f, :] = U[f * group : (f + 1) * group, own]

    for copy in helm_copies():
        copy.wait()
    lrows = up8(levels)
    row = lax.broadcasted_iota(i32, (lrows, group), 0)
    col = lax.broadcasted_iota(i32, (lrows, group), 1)
    c = jnp.zeros((lrows, 1), f32)
    for g in range(nlev):
        c = c + jnp.sum(jnp.where(row - g * group == col, hc[g], 0.0), axis=1, keepdims=True)
    radius = 6.0 * c / (1.0 + 6.0 * c)
    steps = [
        jnp.broadcast_to(
            1.0 / (1.0 + radius * math.cos(math.pi * (2 * j + 1) / (2.0 * SWEEPS))), (lrows, LANES)
        )
        for j in range(SWEEPS)
    ]
    c = jnp.broadcast_to(c, (lrows, LANES))
    nv = lrows // SUB
    to_parts = split(to_modes[...])
    back = from_modes[0:group, :]
    for g in range(1, nlev):
        back = jnp.where(lev == g, from_modes[g * group : (g + 1) * group, :], back)
    back_parts = split(back)

    def modal(b):
        cols = cols_of(b)
        wsum = jnp.sum(lw[:, cols], axis=0, keepdims=True)
        total = product(to_parts, jnp.concatenate([rx[g, :, cols] for g in range(nlev)], axis=0))
        for r in range(nv):
            rows = pl.ds(r * SUB, SUB)
            cr = c[r * SUB : (r + 1) * SUB]
            inv = 1.0 / (1.0 + cr * wsum)
            scaled = total[r * SUB : (r + 1) * SUB] * inv
            rinv[rows, cols] = scaled
            cinv[rows, cols] = cr * inv
            xa[rows, cols] = steps[0][r * SUB : (r + 1) * SUB] * scaled

    def sweep(j, b):
        x_old, x_new = (xa, xb) if j % 2 else (xb, xa)
        cols = cols_of(b)
        own_t, far_t = around(x_old, b, nv)
        acc = [None] * nv
        for k in range(sides):
            lo, here = place(k, b, cols)
            w = row8(lw, k, cols)
            for r in range(nv):
                term = w * jnp.where(here, lanes_of(own_t[r], lo), lanes_of(far_t[r], lo))
                acc[r] = term if acc[r] is None else acc[r] + term
        for r in range(nv):
            rows = pl.ds(r * SUB, SUB)
            s = steps[j][r * SUB : (r + 1) * SUB]
            x_new[rows, cols] = (1.0 - s) * own_t[r] + s * (
                rinv[rows, cols] + cinv[rows, cols] * acc[r]
            )

    x_end = xa if SWEEPS % 2 else xb

    def heights(b):
        height_out[:, cols_of(b - hb)] = product(back_parts, x_end[0:levels, cols_of(b)])

    def off(j):
        return hb - -(-(NBR_REACH * (SWEEPS - 1 - j)) // LANES)

    def finish(side, first_part):
        def part(at, j):
            width = nb_blocks - outer if first_part else outer
            low = (nb_blocks - width) * side
            if j == 0:
                return low, width
            grow = -j if first_part else j
            width = width + grow - at
            return low + jnp.where(side == 0, at, -grow), width

        many = 1 if nv > 4 else nb_blocks
        loop(*part(0, 0), modal, min(many, part(0, 0)[1]))
        for j in range(1, SWEEPS):
            start, count = part(off(j), j)
            loop(start, count, functools.partial(sweep, j), min(many, count))
        start, count = part(hb, SWEEPS - 1)
        loop(start, count, heights, count)

    for copy in lev_copies(0, *inner) + lev_copies(1, begin * (last - 1), outer):
        copy.wait_recv()
    finish(begin, True)
    for copy in lev_copies(2, (1 - begin) * (last - 1), outer):
        copy.wait_recv()
    finish(1 - begin, False)
    for side in (0, 1):
        for copy in halo_copies(side):
            copy.wait_send()
    for copy in lev_copies(0, *inner):
        copy.wait_send()
    for no in (1, 2):
        for copy in lev_copies(no, 0, outer):
            copy.wait_send()


def hand_over(winds_in, height_in, winds_out, height_out, sem):
    copies = [
        pltpu.make_async_copy(winds_in, winds_out, sem.at[0]),
        pltpu.make_async_copy(height_in, height_out, sem.at[1]),
    ]
    for copy in copies:
        copy.start()
    for copy in copies:
        copy.wait()


def per_device(npatch, nlev, *args):
    fields, s_index, _, nbr = args[:4]
    _, group, cells = fields.shape
    points, sides = s_index.shape[0], nbr.shape[0]
    levels = group * nlev
    ext = cells + 2 * HALO
    args = args[:-1] + (args[-1].reshape(1, group),)
    args = [pltpu.with_memory_space_constraint(a, pltpu.HBM) for a in args]
    lrows = up8(levels)
    vm = pltpu.VMEM
    peers = max(nlev - 1, 1)
    winds, height = pl.pallas_call(
        functools.partial(kernel, npatch, nlev),
        out_shape=(
            pltpu.VMEM((group, 2, cells), f32),
            pltpu.VMEM((group, cells), f32),
        ),
        in_specs=[pl.BlockSpec(memory_space=pl.ANY)] * 7
        + [pl.BlockSpec(memory_space=pltpu.VMEM)] * 3,
        out_specs=(
            pl.BlockSpec(memory_space=pltpu.VMEM),
            pl.BlockSpec(memory_space=pltpu.VMEM),
        ),
        scratch_shapes=[vm(a.shape, a.dtype) for a in args[:7]]
        + [
            pltpu.SemaphoreType.DMA((7,)),
            vm((2, 3, group, FIELD_HALO), f32),
            vm((2, points, 1, HALO), i32),
            vm((2, points, 1, HALO), f32),
            vm((2, sides, HALO), i32),
            vm((2, sides, HALO), f32),
            vm((2, sides, HALO), f32),
            vm((2, sides, HALO), f32),
            vm((nlev, 1, group), f32),
            vm((up8(3 * group), cells + 2 * FIELD_HALO + LANES), f32),
            vm((up8(3 * group) * ((cells + 2 * FIELD_HALO) // LANES + 2), 2 * LANES), bf16),
            vm((up8(3 * group) * ((cells + 2 * FIELD_HALO) // LANES + 2), 2 * LANES), bf16),
            vm((points, ext), i32),
            vm((points, ext), f32),
            vm((sides, ext), i32),
            vm((sides, ext), f32),
            vm((sides, ext), f32),
            vm((sides, ext), f32),
            vm((up8(3 * group), ext), f32),
            vm((nlev, group, ext), f32),
            vm((lrows, ext), f32),
            vm((lrows, ext), f32),
            vm((lrows, ext), f32),
            vm((lrows, ext), f32),
            pltpu.SemaphoreType.REGULAR,
            pltpu.SemaphoreType.DMA((14,)),
            pltpu.SemaphoreType.DMA((14,)),
            pltpu.SemaphoreType.DMA((3, peers)),
            pltpu.SemaphoreType.DMA((3, peers)),
            pltpu.SemaphoreType.DMA((peers,)),
            pltpu.SemaphoreType.DMA((peers,)),
        ],
        compiler_params=pltpu.CompilerParams(
            collective_id=0, has_side_effects=True, vmem_limit_bytes=20 << 20
        ),
    )(*args)
    winds, height = pl.pallas_call(
        hand_over,
        out_shape=(
            jax.ShapeDtypeStruct(winds.shape, f32),
            jax.ShapeDtypeStruct(height.shape, f32),
        ),
        in_specs=[pl.BlockSpec(memory_space=pltpu.VMEM)] * 2,
        out_specs=(pl.BlockSpec(memory_space=pl.ANY),) * 2,
        scratch_shapes=[pltpu.SemaphoreType.DMA((2,))],
        compiler_params=pltpu.CompilerParams(vmem_limit_bytes=1 << 20),
    )(winds, height)
    return jnp.transpose(winds, (1, 0, 2)), height


def solution(mesh):
    in_specs = (
        P(None, "lev", "patch"),
        P(None, "lev", "patch"),
        P(None, "lev", "patch"),
        P(None, "patch"),
        P(None, "patch"),
        P(None, "patch"),
        P(None, "patch"),
        P(),
        P(),
        P("lev"),
    )
    out_specs = (P(None, "lev", "patch"), P("lev", "patch"))
    body = functools.partial(per_device, mesh.shape["patch"], mesh.shape["lev"])
    return jax.shard_map(
        body, mesh=mesh, in_specs=in_specs, out_specs=out_specs, check_vma=False
    )
```

```python
import functools
import math

import jax
import jax.numpy as jnp
from jax import lax
from jax.experimental import pallas as pl
from jax.experimental.pallas import tpu as pltpu
from jax.sharding import PartitionSpec as P

REACH = 512
NBR_REACH = 64
SWEEPS = 4
COUPLING = 0.5
LANES = 128
SUB = 8
HALO = NBR_REACH * SWEEPS
FIELD_HALO = REACH + HALO
MESH = pl.DeviceIdType.MESH


BITS = LANES.bit_length() - 1
bf16, f32, i32 = jnp.bfloat16, jnp.float32, jnp.int32


def up8(rows):
    return -(-rows // SUB) * SUB


def split(x):
    high = x.astype(bf16)
    return high, (x - high.astype(f32)).astype(bf16)


def product(parts, x):
    high, low = split(x)
    dot = functools.partial(jnp.dot, preferred_element_type=f32)
    return dot(parts[0], high) + (dot(parts[1], high) + dot(parts[0], low))


def lanes_of(x, index):
    return jnp.take_along_axis(x, index, axis=1, mode="promise_in_bounds")


def row8(ref, row, cols):
    return jnp.broadcast_to(ref[pl.ds(row, 1), cols], (SUB, LANES))


def cols_of(block):
    if isinstance(block, int):
        return slice(block * LANES, (block + 1) * LANES)
    return pl.ds(pl.multiple_of(block * LANES, LANES), LANES)


def loop(first, count, body, unroll=1):
    trips = count // unroll

    def step(i, carry):
        for u in range(unroll):
            body(first + i * unroll + u)
        return carry

    if trips == 1:
        step(0, 0)
    else:
        lax.fori_loop(0, trips, step, 0)
    for u in range(trips * unroll, count):
        body(first + u)


def kernel(
    npatch, nlev,
    fields_in, s_index_in, s_weight_in, nbr_in, lap_in, ex_in, ey_in, to_modes, from_modes, helm,
    winds_out, height_out,
    fields, s_index, s_weight, nbr, lap, ex, ey, load_sem,
    f_halo, si_halo, sw_halo, nb_halo, lw_halo, ex_halo, ey_halo, hc,
    F, G, si, sw, nb, lw, gx, gy, U, rx, rinv, cinv, xa, xb,
    near_sem, send_sem, recv_sem, lev_send, lev_recv, hc_send, hc_recv,
):
    group = fields.shape[1]
    cells = fields.shape[2]
    levels = group * nlev
    points = s_index.shape[0]
    sides = nbr.shape[0]
    ext = cells + 2 * HALO
    nb_blocks = ext // LANES
    own_blocks = cells // LANES
    hb = HALO // LANES
    patch = lax.axis_index("patch")
    lev = lax.axis_index("lev")
    right = lax.rem(patch + 1, npatch)
    left = lax.rem(patch + npatch - 1, npatch)

    barrier = pltpu.get_barrier_semaphore()
    pl.semaphore_signal(barrier, inc=1, device_id={"patch": right}, device_id_type=MESH)

    @pl.when(patch != 1)
    def _():
        pl.semaphore_signal(barrier, inc=1, device_id={"patch": left}, device_id_type=MESH)

    for d in range(1, nlev):
        pl.semaphore_signal(
            barrier, inc=1, device_id={"lev": lax.rem(lev + d, nlev)}, device_id_type=MESH
        )
    loads = []
    for no, (src, dst) in enumerate((
        (fields_in, fields), (s_index_in, s_index), (s_weight_in, s_weight),
        (nbr_in, nbr), (lap_in, lap), (ex_in, ex), (ey_in, ey),
    )):
        copy = pltpu.make_async_copy(src, dst, load_sem.at[no])
        copy.start()
        loads.append(copy)
    hc[lev] = helm[...]

    pairs = (
        (s_index_in, si_halo, HALO),
        (s_weight_in, sw_halo, HALO),
        (fields_in, f_halo, FIELD_HALO),
        (nbr_in, nb_halo, HALO),
        (ex_in, ex_halo, HALO),
        (ey_in, ey_halo, HALO),
        (lap_in, lw_halo, HALO),
    )

    def halo_copies(side):
        made = []
        for no, (src, dst, width) in enumerate(pairs):
            lead = (slice(None),) * (len(src.shape) - 1)
            start = (1 - side) * (cells - width)
            if not isinstance(side, int):
                start = pl.multiple_of(start, LANES)
            made.append(pltpu.make_async_remote_copy(
                src_ref=src.at[lead + (pl.ds(start, width),)],
                dst_ref=dst.at[side],
                send_sem=send_sem.at[2 * no + side],
                recv_sem=recv_sem.at[2 * no + side],
                device_id={"patch": lax.rem(patch + npatch + 1 - 2 * side, npatch)},
                device_id_type=MESH,
            ))
        return made

    def helm_copies():
        return [
            pltpu.make_async_remote_copy(
                src_ref=helm,
                dst_ref=hc.at[lev],
                send_sem=hc_send.at[d - 1],
                recv_sem=hc_recv.at[d - 1],
                device_id={"lev": lax.rem(lev + d, nlev)},
                device_id_type=MESH,
            )
            for d in range(1, nlev)
        ]

    def start(made):
        for copy in made:
            copy.start()

    @pl.when(patch != 0)
    def _():
        pl.semaphore_wait(barrier, 2 + nlev - 1)

    @pl.when(patch == 1)
    def _():
        pl.semaphore_signal(near_sem, inc=1, device_id={"patch": left}, device_id_type=MESH)

    @pl.when(patch != 0)
    def _():
        start(halo_copies(0) + halo_copies(1) + helm_copies())

    frows = F.shape[0]
    tiles = 2 * REACH // LANES + 1
    ftiles = F.shape[1] // LANES
    own_lo = FIELD_HALO // LANES
    own_hi = own_lo + own_blocks

    def tile_rows(tile, count, odd):
        start = tile * frows + odd * (G.shape[0] // 2 + frows % (2 * SUB))
        if not isinstance(start, int):
            start = pl.multiple_of(start, 2 * SUB)
        return pl.ds(start, count * frows)

    def split_pair(tile, odd):
        rows = tile_rows(tile, 2, odd)
        high, low = split(
            jnp.concatenate([F[:, cols_of(tile)], F[:, cols_of(tile + 1)]], axis=0)
        )
        G[rows, 0:LANES] = high
        G[rows, LANES : 2 * LANES] = low

    lane_id = lax.broadcasted_iota(i32, (LANES, LANES), 0).astype(f32).astype(bf16)
    one = jnp.ones((LANES, LANES), bf16)
    zero = jnp.zeros((LANES, LANES), bf16)

    def upstream(b, odd, t0=0, count=tiles, by_lane=(2, 5), add=False):
        cols = cols_of(b)
        nv = frows // SUB
        acc = [None] * nv
        field = G.at[tile_rows(b + t0, count, odd), :]
        for pair_no in range(points // 2):
            pair = (2 * pair_no, 2 * pair_no + 1)
            his, los = [], []
            for q in pair:
                x = row8(si, q, cols)
                his.append((x >> BITS) - b)
                los.append(x & (LANES - 1))
            on_lanes = pair_no in by_lane
            if not on_lanes:
                got = jnp.dot(field[...], one_hot(los), preferred_element_type=f32)
            for no, q in enumerate(pair):
                w = row8(sw, q, cols)
                here = [his[no] - t0 == t for t in range(count)]
                for r in range(nv):
                    sel = None if count == tiles else jnp.zeros((SUB, LANES), f32)
                    for t in range(count):
                        row = t * frows + r * SUB
                        if on_lanes:
                            taken = lanes_of(
                                F[r * SUB : (r + 1) * SUB, cols_of(b + t0 + t)], los[no]
                            )
                        else:
                            taken = got[row : row + SUB, no * LANES : (no + 1) * LANES]
                        sel = taken if sel is None else jnp.where(here[t], taken, sel)
                    acc[r] = w * sel if acc[r] is None else acc[r] + w * sel
        for r in range(nv):
            at = slice(r * SUB, (r + 1) * SUB)
            U[at, cols] = U[at, cols] + acc[r] if add else acc[r]

    lane = lax.broadcasted_iota(i32, (SUB, LANES), 1)
    low_half = lane < NBR_REACH

    def around(ref, b, nvregs):
        before = jnp.maximum(b - 1, 0)
        after = jnp.minimum(b + 1, nb_blocks - 1)
        own_tiles, far_tiles = [], []
        for r in range(nvregs):
            rows = pl.ds(r * SUB, SUB)
            own_tiles.append(ref[rows, cols_of(b)])
            far_tiles.append(
                jnp.where(low_half, ref[rows, cols_of(after)], ref[rows, cols_of(before)])
            )
        return own_tiles, far_tiles

    def place(k, b, cols):
        x = row8(nb, k, cols)
        return x & (LANES - 1), (x >> BITS) == b

    def one_hot(los):
        hot = []
        for lo in los:
            lo = jnp.broadcast_to(lo[0:1].astype(f32), (LANES, LANES))
            h = jnp.where(lane_id == lo.astype(bf16), one, zero)
            hot.append(jnp.concatenate([h, h], axis=0))
        return jnp.concatenate(hot, axis=1)

    def beside(own_t, far_t, b, cols):
        nv = len(own_t)
        places = [place(k, b, cols) for k in range(sides)]
        by_product = range(sides - 2, sides)
        if len(by_product):
            high, low = split(jnp.concatenate(own_t + far_t, axis=0))
            got = jnp.dot(
                jnp.concatenate([high, low], axis=1),
                one_hot([places[k][0] for k in by_product]),
                preferred_element_type=f32,
            )
        for k in range(sides):
            lo, here = places[k]
            for r in range(nv):
                if k in by_product:
                    at = (k - by_product[0]) * LANES
                    mine = got[r * SUB : (r + 1) * SUB, at : at + LANES]
                    far = got[(nv + r) * SUB : (nv + r + 1) * SUB, at : at + LANES]
                else:
                    mine, far = lanes_of(own_t[r], lo), lanes_of(far_t[r], lo)
                yield k, r, jnp.where(here, mine, far)

    wrows = up8(2 * group)
    sub_iota = lax.broadcasted_iota(i32, (SUB, LANES), 0)

    def right_side(b):
        cols = cols_of(b)
        nv = wrows // SUB
        own_t, far_t = around(U, b, nv)
        acc = [jnp.zeros((SUB, LANES), f32)] * nv
        for k, r, taken in beside(own_t, far_t, b, cols):
            wx, wy = row8(gx, k, cols), row8(gy, k, cols)
            if (r + 1) * SUB <= group:
                w = wx
            elif r * SUB >= group:
                w = wy
            else:
                w = jnp.where(sub_iota + r * SUB < group, wx, wy)
            acc[r] = acc[r] + w * (taken - own_t[r])
        both = jnp.concatenate(acc, axis=0)
        div = both[0:group] + both[group : 2 * group]
        rx[lev, :, cols] = U[2 * group : 3 * group, cols] - COUPLING * div

    first = hb + REACH // LANES
    last = nb_blocks - first
    inner = (first + 1, last - first - 2)
    outer = first + 1

    def lev_copies(no, at, count):
        at = pl.ds(at * LANES if isinstance(at, int) else pl.multiple_of(at * LANES, LANES), count * LANES)
        return [
            pltpu.make_async_remote_copy(
                src_ref=rx.at[lev, :, at],
                dst_ref=rx.at[lev, :, at],
                send_sem=lev_send.at[no, d - 1],
                recv_sem=lev_recv.at[no, d - 1],
                device_id={"lev": lax.rem(lev + d, nlev)},
                device_id_type=MESH,
            )
            for d in range(1, nlev)
        ]

    def arrive(side):
        for copy in halo_copies(side):
            copy.wait_recv()
        at = pl.ds(pl.multiple_of(side * (FIELD_HALO + cells), LANES), FIELD_HALO)
        for f in range(3):
            F[f * group : (f + 1) * group, at] = f_halo[side, f]
        for i in range(0, own_lo, 2):
            split_pair(side * own_hi + i, 0)
        for i in range(1, own_lo + 2, 2):
            split_pair(side * (own_hi - 2) + i, 1)
        at = pl.ds(pl.multiple_of(side * (HALO + cells), LANES), HALO)
        shift = HALO + (2 * side - 1) * cells
        si[:, at] = si_halo[side, :, 0, :] + shift
        sw[:, at] = sw_halo[side, :, 0, :]
        nb[:, at] = nb_halo[side] + (shift - NBR_REACH)
        lw[:, at] = lw_halo[side]
        gx[:, at] = ex_halo[side]
        gy[:, at] = ey_halo[side]

    for copy in loads:
        copy.wait()
    for f in range(3):
        F[f * group : (f + 1) * group, FIELD_HALO : FIELD_HALO + cells] = fields[f]
    own = slice(HALO, HALO + cells)
    si[:, own] = s_index[:, 0, :] + HALO
    sw[:, own] = s_weight[:, 0, :]
    for tile in range(own_lo, own_hi, 2):
        split_pair(tile, 0)
    for tile in range(own_lo + 1, own_hi, 2):
        split_pair(tile, 1)
    middle = first + 2
    for b in range(first, middle):
        upstream(b, b % 2)

    @pl.when(patch == 0)
    def _():
        pl.semaphore_wait(near_sem, 1)
        start(halo_copies(0))

    for b in range(middle, last):
        upstream(b, b % 2)
    nb[:, own] = nbr[...] + (HALO - NBR_REACH)
    lw[:, own] = lap[...]
    gx[:, own] = ex[...]
    gy[:, own] = ey[...]

    @pl.when(patch == 0)
    def _():
        pl.semaphore_wait(barrier, 2 + nlev - 2)
        start(halo_copies(1) + helm_copies())

    loop(*inner, right_side, inner[1])
    for copy in lev_copies(0, *inner):
        copy.start()
    begin = 1 - lax.rem(patch, 2)

    def flank(side, turn):
        arrive(side)
        if turn == 0:
            for i in range(first):
                upstream(side * last + i, i % 2)
        else:
            for i in range(hb):
                upstream(side * (nb_blocks - hb) + i, i % 2, by_lane=())
            for m in range(mixed):
                upstream(near(side, m), 0, side * (tiles - 1 - m), m + 1, range(points), True)
        loop(side * (last - 1), outer, right_side, outer)
        for copy in lev_copies(1 + turn, side * (last - 1), outer):
            copy.start()

    mixed = first - hb

    def near(side, m):
        return first - 1 - m + side * (last - first + 1 + 2 * m)

    flank(begin, 0)
    side = 1 - begin
    for m in range(mixed):
        b, t0 = near(side, m), (1 - side) * (m + 1)
        upstream(b, lax.rem(b + t0, 2), t0, tiles - 1 - m)
    flank(side, 1)

    for f in range(2):
        winds_out[:, f, :] = U[f * group : (f + 1) * group, own]

    for copy in helm_copies():
        copy.wait()
    lrows = up8(levels)
    row = lax.broadcasted_iota(i32, (lrows, group), 0)
    col = lax.broadcasted_iota(i32, (lrows, group), 1)
    c = jnp.zeros((lrows, 1), f32)
    for g in range(nlev):
        c = c + jnp.sum(jnp.where(row - g * group == col, hc[g], 0.0), axis=1, keepdims=True)
    radius = 6.0 * c / (1.0 + 6.0 * c)
    steps = [
        jnp.broadcast_to(
            1.0 / (1.0 + radius * math.cos(math.pi * (2 * j + 1) / (2.0 * SWEEPS))), (lrows, LANES)
        )
        for j in range(SWEEPS)
    ]
    c = jnp.broadcast_to(c, (lrows, LANES))
    nv = lrows // SUB
    to_parts = split(to_modes[...])
    back = from_modes[0:group, :]
    for g in range(1, nlev):
        back = jnp.where(lev == g, from_modes[g * group : (g + 1) * group, :], back)
    back_parts = split(back)

    def modal(b):
        cols = cols_of(b)
        wsum = jnp.sum(lw[:, cols], axis=0, keepdims=True)
        total = product(to_parts, jnp.concatenate([rx[g, :, cols] for g in range(nlev)], axis=0))
        for r in range(nv):
            rows = pl.ds(r * SUB, SUB)
            cr = c[r * SUB : (r + 1) * SUB]
            inv = 1.0 / (1.0 + cr * wsum)
            scaled = total[r * SUB : (r + 1) * SUB] * inv
            rinv[rows, cols] = scaled
            cinv[rows, cols] = cr * inv
            xa[rows, cols] = steps[0][r * SUB : (r + 1) * SUB] * scaled

    def sweep(j, b):
        x_old, x_new = (xa, xb) if j % 2 else (xb, xa)
        cols = cols_of(b)
        own_t, far_t = around(x_old, b, nv)
        acc = [None] * nv
        for k, r, taken in beside(own_t, far_t, b, cols):
            term = row8(lw, k, cols) * taken
            acc[r] = term if acc[r] is None else acc[r] + term
        for r in range(nv):
            rows = pl.ds(r * SUB, SUB)
            s = steps[j][r * SUB : (r + 1) * SUB]
            x_new[rows, cols] = (1.0 - s) * own_t[r] + s * (
                rinv[rows, cols] + cinv[rows, cols] * acc[r]
            )

    x_end = xa if SWEEPS % 2 else xb

    def heights(b):
        height_out[:, cols_of(b - hb)] = product(back_parts, x_end[0:levels, cols_of(b)])

    def off(j):
        return hb - -(-(NBR_REACH * (SWEEPS - 1 - j)) // LANES)

    def finish(side, first_part):
        def part(at, j):
            width = nb_blocks - outer if first_part else outer
            low = (nb_blocks - width) * side
            if j == 0:
                return low, width
            grow = -j if first_part else j
            width = width + grow - at
            return low + jnp.where(side == 0, at, -grow), width

        many = 1 if nv > 4 else nb_blocks
        loop(*part(0, 0), modal, min(many, part(0, 0)[1]))
        for j in range(1, SWEEPS):
            start, count = part(off(j), j)
            loop(start, count, functools.partial(sweep, j), min(many, count))
        start, count = part(hb, SWEEPS - 1)
        loop(start, count, heights, count)

    for copy in lev_copies(0, *inner) + lev_copies(1, begin * (last - 1), outer):
        copy.wait_recv()
    finish(begin, True)
    for copy in lev_copies(2, (1 - begin) * (last - 1), outer):
        copy.wait_recv()
    finish(1 - begin, False)
    for side in (0, 1):
        for copy in halo_copies(side):
            copy.wait_send()
    for copy in lev_copies(0, *inner):
        copy.wait_send()
    for no in (1, 2):
        for copy in lev_copies(no, 0, outer):
            copy.wait_send()


def hand_over(winds_in, height_in, winds_out, height_out, sem):
    copies = [
        pltpu.make_async_copy(winds_in, winds_out, sem.at[0]),
        pltpu.make_async_copy(height_in, height_out, sem.at[1]),
    ]
    for copy in copies:
        copy.start()
    for copy in copies:
        copy.wait()


def per_device(npatch, nlev, *args):
    fields, s_index, _, nbr = args[:4]
    _, group, cells = fields.shape
    points, sides = s_index.shape[0], nbr.shape[0]
    levels = group * nlev
    ext = cells + 2 * HALO
    args = args[:-1] + (args[-1].reshape(1, group),)
    args = [pltpu.with_memory_space_constraint(a, pltpu.HBM) for a in args]
    lrows = up8(levels)
    vm = pltpu.VMEM
    peers = max(nlev - 1, 1)
    winds, height = pl.pallas_call(
        functools.partial(kernel, npatch, nlev),
        out_shape=(
            pltpu.VMEM((group, 2, cells), f32),
            pltpu.VMEM((group, cells), f32),
        ),
        in_specs=[pl.BlockSpec(memory_space=pl.ANY)] * 7
        + [pl.BlockSpec(memory_space=pltpu.VMEM)] * 3,
        out_specs=(
            pl.BlockSpec(memory_space=pltpu.VMEM),
            pl.BlockSpec(memory_space=pltpu.VMEM),
        ),
        scratch_shapes=[vm(a.shape, a.dtype) for a in args[:7]]
        + [
            pltpu.SemaphoreType.DMA((7,)),
            vm((2, 3, group, FIELD_HALO), f32),
            vm((2, points, 1, HALO), i32),
            vm((2, points, 1, HALO), f32),
            vm((2, sides, HALO), i32),
            vm((2, sides, HALO), f32),
            vm((2, sides, HALO), f32),
            vm((2, sides, HALO), f32),
            vm((nlev, 1, group), f32),
            vm((up8(3 * group), cells + 2 * FIELD_HALO + LANES), f32),
            vm((2 * up8(3 * group) * ((cells + 2 * FIELD_HALO) // LANES + 2), 2 * LANES), bf16),
            vm((points, ext), i32),
            vm((points, ext), f32),
            vm((sides, ext), i32),
            vm((sides, ext), f32),
            vm((sides, ext), f32),
            vm((sides, ext), f32),
            vm((up8(3 * group), ext), f32),
            vm((nlev, group, ext), f32),
            vm((lrows, ext), f32),
            vm((lrows, ext), f32),
            vm((lrows, ext), f32),
            vm((lrows, ext), f32),
            pltpu.SemaphoreType.REGULAR,
            pltpu.SemaphoreType.DMA((14,)),
            pltpu.SemaphoreType.DMA((14,)),
            pltpu.SemaphoreType.DMA((3, peers)),
            pltpu.SemaphoreType.DMA((3, peers)),
            pltpu.SemaphoreType.DMA((peers,)),
            pltpu.SemaphoreType.DMA((peers,)),
        ],
        compiler_params=pltpu.CompilerParams(
            collective_id=0, has_side_effects=True, vmem_limit_bytes=20 << 20
        ),
    )(*args)
    winds, height = pl.pallas_call(
        hand_over,
        out_shape=(
            jax.ShapeDtypeStruct(winds.shape, f32),
            jax.ShapeDtypeStruct(height.shape, f32),
        ),
        in_specs=[pl.BlockSpec(memory_space=pltpu.VMEM)] * 2,
        out_specs=(pl.BlockSpec(memory_space=pl.ANY),) * 2,
        scratch_shapes=[pltpu.SemaphoreType.DMA((2,))],
        compiler_params=pltpu.CompilerParams(vmem_limit_bytes=1 << 20),
    )(winds, height)
    return jnp.transpose(winds, (1, 0, 2)), height


def solution(mesh):
    in_specs = (
        P(None, "lev", "patch"),
        P(None, "lev", "patch"),
        P(None, "lev", "patch"),
        P(None, "patch"),
        P(None, "patch"),
        P(None, "patch"),
        P(None, "patch"),
        P(),
        P(),
        P("lev"),
    )
    out_specs = (P(None, "lev", "patch"), P("lev", "patch"))
    body = functools.partial(per_device, mesh.shape["patch"], mesh.shape["lev"])
    return jax.shard_map(
        body, mesh=mesh, in_specs=in_specs, out_specs=out_specs, check_vma=False
    )
```

```python
import functools
import math

import jax
import jax.numpy as jnp
from jax import lax
from jax.experimental import pallas as pl
from jax.experimental.pallas import tpu as pltpu
from jax.sharding import PartitionSpec as P

REACH = 512
NBR_REACH = 64
SWEEPS = 4
COUPLING = 0.5
LANES = 128
SUB = 8
HALO = NBR_REACH * SWEEPS
FIELD_HALO = REACH + HALO
MESH = pl.DeviceIdType.MESH


BITS = LANES.bit_length() - 1
bf16, f32, i32 = jnp.bfloat16, jnp.float32, jnp.int32


def up8(rows):
    return -(-rows // SUB) * SUB


def split(x):
    high = x.astype(bf16)
    return high, (x - high.astype(f32)).astype(bf16)


def product(parts, x):
    high, low = split(x)
    dot = functools.partial(jnp.dot, preferred_element_type=f32)
    return dot(parts[0], high) + (dot(parts[1], high) + dot(parts[0], low))


def lanes_of(x, index):
    return jnp.take_along_axis(x, index, axis=1, mode="promise_in_bounds")


def row8(ref, row, cols):
    return jnp.broadcast_to(ref[pl.ds(row, 1), cols], (SUB, LANES))


def cols_of(block):
    if isinstance(block, int):
        return slice(block * LANES, (block + 1) * LANES)
    return pl.ds(pl.multiple_of(block * LANES, LANES), LANES)


def loop(first, count, body, unroll=1):
    trips = count // unroll

    def step(i, carry):
        for u in range(unroll):
            body(first + i * unroll + u)
        return carry

    if trips == 1:
        step(0, 0)
    else:
        lax.fori_loop(0, trips, step, 0)
    for u in range(trips * unroll, count):
        body(first + u)


def kernel(
    npatch, nlev,
    fields_in, s_index_in, s_weight_in, nbr_in, lap_in, ex_in, ey_in, to_modes, from_modes, helm,
    winds_out, height_out,
    fields, s_index, s_weight, nbr, lap, ex, ey, load_sem,
    f_halo, si_halo, sw_halo, nb_halo, lw_halo, ex_halo, ey_halo, hc,
    F, G, L, si, sw, nb, lw, gx, gy, U, rx, rinv, cinv, xa, xb, xs0, xs1,
    near_sem, send_sem, recv_sem, lev_send, lev_recv, hc_send, hc_recv,
):
    group = fields.shape[1]
    cells = fields.shape[2]
    levels = group * nlev
    points = s_index.shape[0]
    sides = nbr.shape[0]
    ext = cells + 2 * HALO
    nb_blocks = ext // LANES
    own_blocks = cells // LANES
    hb = HALO // LANES
    patch = lax.axis_index("patch")
    lev = lax.axis_index("lev")
    right = lax.rem(patch + 1, npatch)
    left = lax.rem(patch + npatch - 1, npatch)

    barrier = pltpu.get_barrier_semaphore()
    pl.semaphore_signal(barrier, inc=1, device_id={"patch": right}, device_id_type=MESH)

    @pl.when(patch != 1)
    def _():
        pl.semaphore_signal(barrier, inc=1, device_id={"patch": left}, device_id_type=MESH)

    for d in range(1, nlev):
        pl.semaphore_signal(
            barrier, inc=1, device_id={"lev": lax.rem(lev + d, nlev)}, device_id_type=MESH
        )
    loads = []
    for no, (src, dst) in enumerate((
        (fields_in, fields), (s_index_in, s_index), (s_weight_in, s_weight),
        (nbr_in, nbr), (lap_in, lap), (ex_in, ex), (ey_in, ey),
    )):
        copy = pltpu.make_async_copy(src, dst, load_sem.at[no])
        copy.start()
        loads.append(copy)
    hc[lev] = helm[...]

    pairs = (
        (s_index_in, si_halo, HALO),
        (s_weight_in, sw_halo, HALO),
        (fields_in, f_halo, FIELD_HALO),
        (nbr_in, nb_halo, HALO),
        (ex_in, ex_halo, HALO),
        (ey_in, ey_halo, HALO),
        (lap_in, lw_halo, HALO),
    )

    def halo_copies(side):
        made = []
        for no, (src, dst, width) in enumerate(pairs):
            lead = (slice(None),) * (len(src.shape) - 1)
            start = (1 - side) * (cells - width)
            if not isinstance(side, int):
                start = pl.multiple_of(start, LANES)
            made.append(pltpu.make_async_remote_copy(
                src_ref=src.at[lead + (pl.ds(start, width),)],
                dst_ref=dst.at[side],
                send_sem=send_sem.at[2 * no + side],
                recv_sem=recv_sem.at[2 * no + side],
                device_id={"patch": lax.rem(patch + npatch + 1 - 2 * side, npatch)},
                device_id_type=MESH,
            ))
        return made

    def helm_copies():
        return [
            pltpu.make_async_remote_copy(
                src_ref=helm,
                dst_ref=hc.at[lev],
                send_sem=hc_send.at[d - 1],
                recv_sem=hc_recv.at[d - 1],
                device_id={"lev": lax.rem(lev + d, nlev)},
                device_id_type=MESH,
            )
            for d in range(1, nlev)
        ]

    def start(made):
        for copy in made:
            copy.start()

    @pl.when(patch != 0)
    def _():
        pl.semaphore_wait(barrier, 2 + nlev - 1)

    @pl.when(patch == 1)
    def _():
        pl.semaphore_signal(near_sem, inc=1, device_id={"patch": left}, device_id_type=MESH)

    @pl.when(patch != 0)
    def _():
        start(halo_copies(0) + halo_copies(1) + helm_copies())

    frows = F.shape[0]
    tiles = 2 * REACH // LANES + 1
    ftiles = F.shape[1] // LANES
    own_lo = FIELD_HALO // LANES
    own_hi = own_lo + own_blocks

    def tile_rows(tile, count, odd):
        start = tile * frows + odd * (G.shape[0] // 2 + frows % (2 * SUB))
        if not isinstance(start, int):
            start = pl.multiple_of(start, 2 * SUB)
        return pl.ds(start, count * frows)

    def split_pair(tile, odd):
        rows = tile_rows(tile, 2, odd)
        high, low = split(
            jnp.concatenate([F[:, cols_of(tile)], F[:, cols_of(tile + 1)]], axis=0)
        )
        G[rows, 0:LANES] = high
        G[rows, LANES : 2 * LANES] = low

    lane_id = lax.broadcasted_iota(i32, (LANES, LANES), 0).astype(f32).astype(bf16)
    one = jnp.ones((LANES, LANES), bf16)
    zero = jnp.zeros((LANES, LANES), bf16)

    def upstream(b, odd, t0=0, count=tiles, by_lane=(2, 5), add=False):
        cols = cols_of(b)
        nv = frows // SUB
        acc = [None] * nv
        field = G.at[tile_rows(b + t0, count, odd), :]
        for pair_no in range(points // 2):
            pair = (2 * pair_no, 2 * pair_no + 1)
            his, los = [], []
            for q in pair:
                x = row8(si, q, cols)
                his.append((x >> BITS) - b)
                los.append(x & (LANES - 1))
            on_lanes = pair_no in by_lane
            if not on_lanes:
                got = jnp.dot(field[...], one_hot(los), preferred_element_type=f32)
            for no, q in enumerate(pair):
                w = row8(sw, q, cols)
                here = [his[no] - t0 == t for t in range(count)]
                for r in range(nv):
                    sel = None if count == tiles else jnp.zeros((SUB, LANES), f32)
                    for t in range(count):
                        row = t * frows + r * SUB
                        if on_lanes:
                            taken = lanes_of(
                                F[r * SUB : (r + 1) * SUB, cols_of(b + t0 + t)], los[no]
                            )
                        else:
                            taken = got[row : row + SUB, no * LANES : (no + 1) * LANES]
                        sel = taken if sel is None else jnp.where(here[t], taken, sel)
                    acc[r] = w * sel if acc[r] is None else acc[r] + w * sel
        for r in range(nv):
            at = slice(r * SUB, (r + 1) * SUB)
            U[at, cols] = U[at, cols] + acc[r] if add else acc[r]

    lane = lax.broadcasted_iota(i32, (SUB, LANES), 1)
    low_half = lane < NBR_REACH

    def around(ref, b, nvregs):
        before = jnp.maximum(b - 1, 0)
        after = jnp.minimum(b + 1, nb_blocks - 1)
        own_tiles, far_tiles = [], []
        for r in range(nvregs):
            rows = pl.ds(r * SUB, SUB)
            own_tiles.append(ref[rows, cols_of(b)])
            far_tiles.append(
                jnp.where(low_half, ref[rows, cols_of(after)], ref[rows, cols_of(before)])
            )
        return own_tiles, far_tiles

    def place(k, b, cols):
        x = row8(nb, k, cols)
        return x & (LANES - 1), (x >> BITS) == b

    window_id = lax.broadcasted_iota(i32, (2 * LANES, LANES), 0).astype(f32).astype(bf16)

    def wide(x):
        return jnp.broadcast_to(x[0:1], (2 * LANES, LANES)).astype(bf16)

    def neighbour_matrix(b):
        cols = cols_of(b)
        at, weight = [], []
        for q in range(sides):
            lo, here = place(q, b, cols)
            at.append(jnp.where(here, lo, lo + LANES))
            weight.append(row8(lw, q, cols))
        for q in range(sides):
            for p in range(q + 1, sides):
                weight[q] = weight[q] + jnp.where(at[q] == at[p], row8(lw, p, cols), 0.0)
        high = jnp.zeros((2 * LANES, LANES), bf16)
        low = jnp.zeros((2 * LANES, LANES), bf16)
        for q in reversed(range(sides)):
            w_high = weight[q].astype(bf16).astype(f32)
            hit = window_id == wide(at[q].astype(f32))
            high = jnp.where(hit, wide(w_high), high)
            low = jnp.where(hit, wide(weight[q] - w_high), low)
        L[b, :, 0:LANES] = high
        L[b, :, LANES : 2 * LANES] = low

    def one_hot(los):
        hot = []
        for lo in los:
            lo = jnp.broadcast_to(lo[0:1].astype(f32), (LANES, LANES))
            h = jnp.where(lane_id == lo.astype(bf16), one, zero)
            hot.append(jnp.concatenate([h, h], axis=0))
        return jnp.concatenate(hot, axis=1)

    def beside(own_t, far_t, b, cols):
        nv = len(own_t)
        places = [place(k, b, cols) for k in range(sides)]
        by_product = range(sides - 2, sides)
        if len(by_product):
            high, low = split(jnp.concatenate(own_t + far_t, axis=0))
            got = jnp.dot(
                jnp.concatenate([high, low], axis=1),
                one_hot([places[k][0] for k in by_product]),
                preferred_element_type=f32,
            )
        for k in range(sides):
            lo, here = places[k]
            for r in range(nv):
                if k in by_product:
                    at = (k - by_product[0]) * LANES
                    mine = got[r * SUB : (r + 1) * SUB, at : at + LANES]
                    far = got[(nv + r) * SUB : (nv + r + 1) * SUB, at : at + LANES]
                else:
                    mine, far = lanes_of(own_t[r], lo), lanes_of(far_t[r], lo)
                yield k, r, jnp.where(here, mine, far)

    wrows = up8(2 * group)
    sub_iota = lax.broadcasted_iota(i32, (SUB, LANES), 0)

    def right_side(b):
        cols = cols_of(b)
        nv = wrows // SUB
        own_t, far_t = around(U, b, nv)
        acc = [jnp.zeros((SUB, LANES), f32)] * nv
        for k, r, taken in beside(own_t, far_t, b, cols):
            wx, wy = row8(gx, k, cols), row8(gy, k, cols)
            if (r + 1) * SUB <= group:
                w = wx
            elif r * SUB >= group:
                w = wy
            else:
                w = jnp.where(sub_iota + r * SUB < group, wx, wy)
            acc[r] = acc[r] + w * (taken - own_t[r])
        both = jnp.concatenate(acc, axis=0)
        div = both[0:group] + both[group : 2 * group]
        rx[lev, :, cols] = U[2 * group : 3 * group, cols] - COUPLING * div

    first = hb + REACH // LANES
    last = nb_blocks - first
    inner = (first + 1, last - first - 2)
    outer = first + 1

    def lev_copies(no, at, count):
        at = pl.ds(at * LANES if isinstance(at, int) else pl.multiple_of(at * LANES, LANES), count * LANES)
        return [
            pltpu.make_async_remote_copy(
                src_ref=rx.at[lev, :, at],
                dst_ref=rx.at[lev, :, at],
                send_sem=lev_send.at[no, d - 1],
                recv_sem=lev_recv.at[no, d - 1],
                device_id={"lev": lax.rem(lev + d, nlev)},
                device_id_type=MESH,
            )
            for d in range(1, nlev)
        ]

    def arrive(side):
        for copy in halo_copies(side):
            copy.wait_recv()
        at = pl.ds(pl.multiple_of(side * (FIELD_HALO + cells), LANES), FIELD_HALO)
        for f in range(3):
            F[f * group : (f + 1) * group, at] = f_halo[side, f]
        for i in range(0, own_lo, 2):
            split_pair(side * own_hi + i, 0)
        for i in range(1, own_lo + 2, 2):
            split_pair(side * (own_hi - 2) + i, 1)
        at = pl.ds(pl.multiple_of(side * (HALO + cells), LANES), HALO)
        shift = HALO + (2 * side - 1) * cells
        si[:, at] = si_halo[side, :, 0, :] + shift
        sw[:, at] = sw_halo[side, :, 0, :]
        nb[:, at] = nb_halo[side] + (shift - NBR_REACH)
        lw[:, at] = lw_halo[side]
        gx[:, at] = ex_halo[side]
        gy[:, at] = ey_halo[side]

    for copy in loads:
        copy.wait()
    for f in range(3):
        F[f * group : (f + 1) * group, FIELD_HALO : FIELD_HALO + cells] = fields[f]
    own = slice(HALO, HALO + cells)
    si[:, own] = s_index[:, 0, :] + HALO
    sw[:, own] = s_weight[:, 0, :]
    for tile in range(own_lo, own_hi, 2):
        split_pair(tile, 0)
    for tile in range(own_lo + 1, own_hi, 2):
        split_pair(tile, 1)
    nb[:, own] = nbr[...] + (HALO - NBR_REACH)
    lw[:, own] = lap[...]
    gx[:, own] = ex[...]
    gy[:, own] = ey[...]
    middle = first + 2
    for b in range(first, middle):
        upstream(b, b % 2)
        neighbour_matrix(b)

    @pl.when(patch == 0)
    def _():
        pl.semaphore_wait(near_sem, 1)
        start(halo_copies(0))

    for b in range(middle, last):
        upstream(b, b % 2)
        neighbour_matrix(b)

    @pl.when(patch == 0)
    def _():
        pl.semaphore_wait(barrier, 2 + nlev - 2)
        start(halo_copies(1) + helm_copies())

    loop(*inner, right_side, inner[1])
    for copy in lev_copies(0, *inner):
        copy.start()
    begin = 1 - lax.rem(patch, 2)

    def flank(side, turn):
        arrive(side)
        if turn == 0:
            for i in range(first):
                upstream(side * last + i, i % 2)
                neighbour_matrix(side * last + i)
        else:
            for i in range(hb):
                upstream(side * (nb_blocks - hb) + i, i % 2, by_lane=())
                neighbour_matrix(side * (nb_blocks - hb) + i)
            for m in range(mixed):
                upstream(near(side, m), 0, side * (tiles - 1 - m), m + 1, range(points), True)
        loop(side * (last - 1), outer, right_side, outer)
        for copy in lev_copies(1 + turn, side * (last - 1), outer):
            copy.start()

    mixed = first - hb

    def near(side, m):
        return first - 1 - m + side * (last - first + 1 + 2 * m)

    flank(begin, 0)
    side = 1 - begin
    for m in range(mixed):
        b, t0 = near(side, m), (1 - side) * (m + 1)
        upstream(b, lax.rem(b + t0, 2), t0, tiles - 1 - m)
        neighbour_matrix(b)
    flank(side, 1)

    for f in range(2):
        winds_out[:, f, :] = U[f * group : (f + 1) * group, own]

    for copy in helm_copies():
        copy.wait()
    lrows = up8(levels)
    row = lax.broadcasted_iota(i32, (lrows, group), 0)
    col = lax.broadcasted_iota(i32, (lrows, group), 1)
    c = jnp.zeros((lrows, 1), f32)
    for g in range(nlev):
        c = c + jnp.sum(jnp.where(row - g * group == col, hc[g], 0.0), axis=1, keepdims=True)
    radius = 6.0 * c / (1.0 + 6.0 * c)
    steps = [
        jnp.broadcast_to(
            1.0 / (1.0 + radius * math.cos(math.pi * (2 * j + 1) / (2.0 * SWEEPS))), (lrows, LANES)
        )
        for j in range(SWEEPS)
    ]
    c = jnp.broadcast_to(c, (lrows, LANES))
    nv = lrows // SUB
    to_parts = split(to_modes[...])
    back = from_modes[0:group, :]
    for g in range(1, nlev):
        back = jnp.where(lev == g, from_modes[g * group : (g + 1) * group, :], back)
    back_parts = split(back)

    def modal(b):
        cols = cols_of(b)
        wsum = jnp.sum(lw[:, cols], axis=0, keepdims=True)
        new = []
        total = product(to_parts, jnp.concatenate([rx[g, :, cols] for g in range(nlev)], axis=0))
        for r in range(nv):
            rows = pl.ds(r * SUB, SUB)
            cr = c[r * SUB : (r + 1) * SUB]
            inv = 1.0 / (1.0 + cr * wsum)
            scaled = total[r * SUB : (r + 1) * SUB] * inv
            rinv[rows, cols] = scaled
            cinv[rows, cols] = cr * inv
            new.append(steps[0][r * SUB : (r + 1) * SUB] * scaled)
            xa[rows, cols] = new[r]
        xs0[:, cols] = stack(jnp.concatenate(new, axis=0))

    def stack(x):
        return jnp.concatenate([x, x - x.astype(bf16).astype(f32)], axis=0).astype(bf16)

    def sweep(j, b):
        x_old, x_new = (xa, xb) if j % 2 else (xb, xa)
        cols = cols_of(b)
        s_old, s_new = (xs0, xs1) if j % 2 else (xs1, xs0)
        around_b = jnp.where(
            wide_low, s_old[:, cols_of(jnp.minimum(b + 1, nb_blocks - 1))], s_old[:, cols_of(jnp.maximum(b - 1, 0))]
        )
        got = jnp.dot(
            jnp.concatenate([s_old[:, cols], around_b], axis=1), L[b], preferred_element_type=f32
        )
        acc = (got[0:lrows, 0:LANES] + got[0:lrows, LANES:]) + (got[lrows:, 0:LANES] + got[lrows:, LANES:])
        new = []
        for r in range(nv):
            rows = pl.ds(r * SUB, SUB)
            s = steps[j][r * SUB : (r + 1) * SUB]
            new.append((1.0 - s) * x_old[rows, cols] + s * (
                rinv[rows, cols] + cinv[rows, cols] * acc[r * SUB : (r + 1) * SUB]
            ))
            x_new[rows, cols] = new[r]
        if j < SWEEPS - 1:
            s_new[:, cols] = stack(jnp.concatenate(new, axis=0))

    wide_low = lax.broadcasted_iota(i32, (2 * lrows, LANES), 1).astype(f32).astype(bf16) < NBR_REACH

    x_end = xa if SWEEPS % 2 else xb

    def heights(b):
        height_out[:, cols_of(b - hb)] = product(back_parts, x_end[0:levels, cols_of(b)])

    def off(j):
        return hb - -(-(NBR_REACH * (SWEEPS - 1 - j)) // LANES)

    def finish(side, first_part):
        def part(at, j):
            width = nb_blocks - outer if first_part else outer
            low = (nb_blocks - width) * side
            if j == 0:
                return low, width
            grow = -j if first_part else j
            width = width + grow - at
            return low + jnp.where(side == 0, at, -grow), width

        many = 1 if nv > 4 else nb_blocks
        loop(*part(0, 0), modal, min(many, part(0, 0)[1]))
        for j in range(1, SWEEPS):
            start, count = part(off(j), j)
            loop(start, count, functools.partial(sweep, j), min(many, count))
        start, count = part(hb, SWEEPS - 1)
        loop(start, count, heights, count)

    for copy in lev_copies(0, *inner) + lev_copies(1, begin * (last - 1), outer):
        copy.wait_recv()
    finish(begin, True)
    for copy in lev_copies(2, (1 - begin) * (last - 1), outer):
        copy.wait_recv()
    finish(1 - begin, False)
    for side in (0, 1):
        for copy in halo_copies(side):
            copy.wait_send()
    for copy in lev_copies(0, *inner):
        copy.wait_send()
    for no in (1, 2):
        for copy in lev_copies(no, 0, outer):
            copy.wait_send()


def hand_over(winds_in, height_in, winds_out, height_out, sem):
    copies = [
        pltpu.make_async_copy(winds_in, winds_out, sem.at[0]),
        pltpu.make_async_copy(height_in, height_out, sem.at[1]),
    ]
    for copy in copies:
        copy.start()
    for copy in copies:
        copy.wait()


def per_device(npatch, nlev, *args):
    fields, s_index, _, nbr = args[:4]
    _, group, cells = fields.shape
    points, sides = s_index.shape[0], nbr.shape[0]
    levels = group * nlev
    ext = cells + 2 * HALO
    args = args[:-1] + (args[-1].reshape(1, group),)
    args = [pltpu.with_memory_space_constraint(a, pltpu.HBM) for a in args]
    lrows = up8(levels)
    vm = pltpu.VMEM
    peers = max(nlev - 1, 1)
    winds, height = pl.pallas_call(
        functools.partial(kernel, npatch, nlev),
        out_shape=(
            pltpu.VMEM((group, 2, cells), f32),
            pltpu.VMEM((group, cells), f32),
        ),
        in_specs=[pl.BlockSpec(memory_space=pl.ANY)] * 7
        + [pl.BlockSpec(memory_space=pltpu.VMEM)] * 3,
        out_specs=(
            pl.BlockSpec(memory_space=pltpu.VMEM),
            pl.BlockSpec(memory_space=pltpu.VMEM),
        ),
        scratch_shapes=[vm(a.shape, a.dtype) for a in args[:7]]
        + [
            pltpu.SemaphoreType.DMA((7,)),
            vm((2, 3, group, FIELD_HALO), f32),
            vm((2, points, 1, HALO), i32),
            vm((2, points, 1, HALO), f32),
            vm((2, sides, HALO), i32),
            vm((2, sides, HALO), f32),
            vm((2, sides, HALO), f32),
            vm((2, sides, HALO), f32),
            vm((nlev, 1, group), f32),
            vm((up8(3 * group), cells + 2 * FIELD_HALO + LANES), f32),
            vm((2 * up8(3 * group) * ((cells + 2 * FIELD_HALO) // LANES + 2), 2 * LANES), bf16),
            vm((ext // LANES, 2 * LANES, 2 * LANES), bf16),
            vm((points, ext), i32),
            vm((points, ext), f32),
            vm((sides, ext), i32),
            vm((sides, ext), f32),
            vm((sides, ext), f32),
            vm((sides, ext), f32),
            vm((up8(3 * group), ext), f32),
            vm((nlev, group, ext), f32),
            vm((lrows, ext), f32),
            vm((lrows, ext), f32),
            vm((lrows, ext), f32),
            vm((lrows, ext), f32),
            vm((2 * lrows, ext), bf16),
            vm((2 * lrows, ext), bf16),
            pltpu.SemaphoreType.REGULAR,
            pltpu.SemaphoreType.DMA((14,)),
            pltpu.SemaphoreType.DMA((14,)),
            pltpu.SemaphoreType.DMA((3, peers)),
            pltpu.SemaphoreType.DMA((3, peers)),
            pltpu.SemaphoreType.DMA((peers,)),
            pltpu.SemaphoreType.DMA((peers,)),
        ],
        compiler_params=pltpu.CompilerParams(
            collective_id=0, has_side_effects=True, vmem_limit_bytes=20 << 20
        ),
    )(*args)
    winds, height = pl.pallas_call(
        hand_over,
        out_shape=(
            jax.ShapeDtypeStruct(winds.shape, f32),
            jax.ShapeDtypeStruct(height.shape, f32),
        ),
        in_specs=[pl.BlockSpec(memory_space=pltpu.VMEM)] * 2,
        out_specs=(pl.BlockSpec(memory_space=pl.ANY),) * 2,
        scratch_shapes=[pltpu.SemaphoreType.DMA((2,))],
        compiler_params=pltpu.CompilerParams(vmem_limit_bytes=1 << 20),
    )(winds, height)
    return jnp.transpose(winds, (1, 0, 2)), height


def solution(mesh):
    in_specs = (
        P(None, "lev", "patch"),
        P(None, "lev", "patch"),
        P(None, "lev", "patch"),
        P(None, "patch"),
        P(None, "patch"),
        P(None, "patch"),
        P(None, "patch"),
        P(),
        P(),
        P("lev"),
    )
    out_specs = (P(None, "lev", "patch"), P("lev", "patch"))
    body = functools.partial(per_device, mesh.shape["patch"], mesh.shape["lev"])
    return jax.shard_map(
        body, mesh=mesh, in_specs=in_specs, out_specs=out_specs, check_vma=False
    )
```

```python
import functools
import math

import jax
import jax.numpy as jnp
from jax import lax
from jax.experimental import pallas as pl
from jax.experimental.pallas import tpu as pltpu
from jax.sharding import PartitionSpec as P

REACH = 512
NBR_REACH = 64
SWEEPS = 4
COUPLING = 0.5
LANES = 128
SUB = 8
HALO = NBR_REACH * SWEEPS
FIELD_HALO = REACH + HALO
MESH = pl.DeviceIdType.MESH


BITS = LANES.bit_length() - 1
bf16, f32, i32 = jnp.bfloat16, jnp.float32, jnp.int32


def up8(rows):
    return -(-rows // SUB) * SUB


def split(x):
    high = x.astype(bf16)
    return high, (x - high.astype(f32)).astype(bf16)


def product(parts, x):
    high, low = split(x)
    dot = functools.partial(jnp.dot, preferred_element_type=f32)
    return dot(parts[0], high) + (dot(parts[1], high) + dot(parts[0], low))


def lanes_of(x, index):
    return jnp.take_along_axis(x, index, axis=1, mode="promise_in_bounds")


def row8(ref, row, cols):
    return jnp.broadcast_to(ref[pl.ds(row, 1), cols], (SUB, LANES))


def cols_of(block):
    if isinstance(block, int):
        return slice(block * LANES, (block + 1) * LANES)
    return pl.ds(pl.multiple_of(block * LANES, LANES), LANES)


def loop(first, count, body, unroll=1):
    trips = count // unroll

    def step(i, carry):
        for u in range(unroll):
            body(first + i * unroll + u)
        return carry

    if trips == 1:
        step(0, 0)
    else:
        lax.fori_loop(0, trips, step, 0)
    for u in range(trips * unroll, count):
        body(first + u)


def kernel(
    npatch, nlev,
    fields_in, s_index_in, s_weight_in, nbr_in, lap_in, ex_in, ey_in, to_modes, from_modes, helm,
    winds_out, height_out,
    fields, s_index, s_weight, nbr, lap, ex, ey, load_sem,
    f_halo, si_halo, sw_halo, nb_halo, lw_halo, ex_halo, ey_halo, hc,
    F, G, L, si, sw, nb, lw, gx, gy, U, rx, rinv, cinv, xa, xb, xs0, xs1,
    near_sem, send_sem, recv_sem, lev_send, lev_recv, hc_send, hc_recv,
):
    group = fields.shape[1]
    cells = fields.shape[2]
    levels = group * nlev
    points = s_index.shape[0]
    sides = nbr.shape[0]
    ext = cells + 2 * HALO
    nb_blocks = ext // LANES
    own_blocks = cells // LANES
    hb = HALO // LANES
    patch = lax.axis_index("patch")
    lev = lax.axis_index("lev")
    right = lax.rem(patch + 1, npatch)
    left = lax.rem(patch + npatch - 1, npatch)

    barrier = pltpu.get_barrier_semaphore()
    pl.semaphore_signal(barrier, inc=1, device_id={"patch": right}, device_id_type=MESH)

    @pl.when(patch != 1)
    def _():
        pl.semaphore_signal(barrier, inc=1, device_id={"patch": left}, device_id_type=MESH)

    for d in range(1, nlev):
        pl.semaphore_signal(
            barrier, inc=1, device_id={"lev": lax.rem(lev + d, nlev)}, device_id_type=MESH
        )
    loads = []
    for no, (src, dst) in enumerate((
        (fields_in, fields), (s_index_in, s_index), (s_weight_in, s_weight),
        (nbr_in, nbr), (lap_in, lap), (ex_in, ex), (ey_in, ey),
    )):
        copy = pltpu.make_async_copy(src, dst, load_sem.at[no])
        copy.start()
        loads.append(copy)
    hc[lev] = helm[...]

    pairs = (
        (s_index_in, si_halo, HALO),
        (s_weight_in, sw_halo, HALO),
        (fields_in, f_halo, FIELD_HALO),
        (nbr_in, nb_halo, HALO),
        (ex_in, ex_halo, HALO),
        (ey_in, ey_halo, HALO),
        (lap_in, lw_halo, HALO),
    )

    def halo_copies(side, kinds=range(7)):
        made = []
        for no in kinds:
            src, dst, width = pairs[no]
            lead = (slice(None),) * (len(src.shape) - 1)
            start = (1 - side) * (cells - width)
            if not isinstance(side, int):
                start = pl.multiple_of(start, LANES)
            made.append(pltpu.make_async_remote_copy(
                src_ref=src.at[lead + (pl.ds(start, width),)],
                dst_ref=dst.at[side],
                send_sem=send_sem.at[2 * no + side],
                recv_sem=recv_sem.at[2 * no + side],
                device_id={"patch": lax.rem(patch + npatch + 1 - 2 * side, npatch)},
                device_id_type=MESH,
            ))
        return made

    def helm_copies():
        return [
            pltpu.make_async_remote_copy(
                src_ref=helm,
                dst_ref=hc.at[lev],
                send_sem=hc_send.at[d - 1],
                recv_sem=hc_recv.at[d - 1],
                device_id={"lev": lax.rem(lev + d, nlev)},
                device_id_type=MESH,
            )
            for d in range(1, nlev)
        ]

    def start(made):
        for copy in made:
            copy.start()

    @pl.when(patch != 0)
    def _():
        pl.semaphore_wait(barrier, 2 + nlev - 1)

    @pl.when(patch == 1)
    def _():
        pl.semaphore_signal(near_sem, inc=1, device_id={"patch": left}, device_id_type=MESH)

    @pl.when(patch != 0)
    def _():
        start(halo_copies(0) + halo_copies(1) + helm_copies())

    frows = F.shape[0]
    tiles = 2 * REACH // LANES + 1
    ftiles = F.shape[1] // LANES
    own_lo = FIELD_HALO // LANES
    own_hi = own_lo + own_blocks

    def tile_rows(tile, count, odd):
        start = tile * frows + odd * (G.shape[0] // 2 + frows % (2 * SUB))
        if not isinstance(start, int):
            start = pl.multiple_of(start, 2 * SUB)
        return pl.ds(start, count * frows)

    def split_pair(tile, odd):
        rows = tile_rows(tile, 2, odd)
        high, low = split(
            jnp.concatenate([F[:, cols_of(tile)], F[:, cols_of(tile + 1)]], axis=0)
        )
        G[rows, 0:LANES] = high
        G[rows, LANES : 2 * LANES] = low

    lane_id = lax.broadcasted_iota(i32, (LANES, LANES), 0).astype(f32).astype(bf16)
    one = jnp.ones((LANES, LANES), bf16)
    zero = jnp.zeros((LANES, LANES), bf16)

    def upstream(b, odd, t0=0, count=tiles, by_lane=(2, 5), add=False):
        cols = cols_of(b)
        nv = frows // SUB
        acc = [None] * nv
        field = G.at[tile_rows(b + t0, count, odd), :]
        for pair_no in range(points // 2):
            pair = (2 * pair_no, 2 * pair_no + 1)
            his, los = [], []
            for q in pair:
                x = row8(si, q, cols)
                his.append((x >> BITS) - b)
                los.append(x & (LANES - 1))
            on_lanes = pair_no in by_lane
            if not on_lanes:
                got = jnp.dot(field[...], one_hot(los), preferred_element_type=f32)
            for no, q in enumerate(pair):
                w = row8(sw, q, cols)
                here = [his[no] - t0 == t for t in range(count)]
                for r in range(nv):
                    sel = None if count == tiles else jnp.zeros((SUB, LANES), f32)
                    for t in range(count):
                        row = t * frows + r * SUB
                        if on_lanes:
                            taken = lanes_of(
                                F[r * SUB : (r + 1) * SUB, cols_of(b + t0 + t)], los[no]
                            )
                        else:
                            taken = got[row : row + SUB, no * LANES : (no + 1) * LANES]
                        sel = taken if sel is None else jnp.where(here[t], taken, sel)
                    acc[r] = w * sel if acc[r] is None else acc[r] + w * sel
        for r in range(nv):
            at = slice(r * SUB, (r + 1) * SUB)
            U[at, cols] = U[at, cols] + acc[r] if add else acc[r]

    lane = lax.broadcasted_iota(i32, (SUB, LANES), 1)
    low_half = lane < NBR_REACH

    def around(ref, b, nvregs):
        before = jnp.maximum(b - 1, 0)
        after = jnp.minimum(b + 1, nb_blocks - 1)
        own_tiles, far_tiles = [], []
        for r in range(nvregs):
            rows = pl.ds(r * SUB, SUB)
            own_tiles.append(ref[rows, cols_of(b)])
            far_tiles.append(
                jnp.where(low_half, ref[rows, cols_of(after)], ref[rows, cols_of(before)])
            )
        return own_tiles, far_tiles

    def place(k, b, cols):
        x = row8(nb, k, cols)
        return x & (LANES - 1), (x >> BITS) == b

    window_id = lax.broadcasted_iota(i32, (2 * LANES, LANES), 0).astype(f32).astype(bf16)

    def wide(x):
        return jnp.broadcast_to(x[0:1], (2 * LANES, LANES)).astype(bf16)

    def neighbour_matrix(b):
        cols = cols_of(b)
        at, weight = [], []
        for q in range(sides):
            lo, here = place(q, b, cols)
            at.append(jnp.where(here, lo, lo + LANES))
            weight.append(row8(lw, q, cols))
        for q in range(sides):
            for p in range(q + 1, sides):
                weight[q] = weight[q] + jnp.where(at[q] == at[p], row8(lw, p, cols), 0.0)
        high = jnp.zeros((2 * LANES, LANES), bf16)
        low = jnp.zeros((2 * LANES, LANES), bf16)
        for q in reversed(range(sides)):
            w_high = weight[q].astype(bf16).astype(f32)
            hit = window_id == wide(at[q].astype(f32))
            high = jnp.where(hit, wide(w_high), high)
            low = jnp.where(hit, wide(weight[q] - w_high), low)
        L[b, :, 0:LANES] = high
        L[b, :, LANES : 2 * LANES] = low

    def one_hot(los):
        hot = []
        for lo in los:
            lo = jnp.broadcast_to(lo[0:1].astype(f32), (LANES, LANES))
            h = jnp.where(lane_id == lo.astype(bf16), one, zero)
            hot.append(jnp.concatenate([h, h], axis=0))
        return jnp.concatenate(hot, axis=1)

    def beside(own_t, far_t, b, cols):
        nv = len(own_t)
        places = [place(k, b, cols) for k in range(sides)]
        by_product = range(sides - 2, sides)
        if len(by_product):
            high, low = split(jnp.concatenate(own_t + far_t, axis=0))
            got = jnp.dot(
                jnp.concatenate([high, low], axis=1),
                one_hot([places[k][0] for k in by_product]),
                preferred_element_type=f32,
            )
        for k in range(sides):
            lo, here = places[k]
            for r in range(nv):
                if k in by_product:
                    at = (k - by_product[0]) * LANES
                    mine = got[r * SUB : (r + 1) * SUB, at : at + LANES]
                    far = got[(nv + r) * SUB : (nv + r + 1) * SUB, at : at + LANES]
                else:
                    mine, far = lanes_of(own_t[r], lo), lanes_of(far_t[r], lo)
                yield k, r, jnp.where(here, mine, far)

    wrows = up8(2 * group)
    sub_iota = lax.broadcasted_iota(i32, (SUB, LANES), 0)

    def right_side(b):
        cols = cols_of(b)
        nv = wrows // SUB
        own_t, far_t = around(U, b, nv)
        acc = [jnp.zeros((SUB, LANES), f32)] * nv
        for k, r, taken in beside(own_t, far_t, b, cols):
            wx, wy = row8(gx, k, cols), row8(gy, k, cols)
            if (r + 1) * SUB <= group:
                w = wx
            elif r * SUB >= group:
                w = wy
            else:
                w = jnp.where(sub_iota + r * SUB < group, wx, wy)
            acc[r] = acc[r] + w * (taken - own_t[r])
        both = jnp.concatenate(acc, axis=0)
        div = both[0:group] + both[group : 2 * group]
        rx[lev, :, cols] = U[2 * group : 3 * group, cols] - COUPLING * div

    first = hb + REACH // LANES
    last = nb_blocks - first
    inner = (first + 1, last - first - 2)
    outer = first + 1

    def lev_copies(no, at, count):
        at = pl.ds(at * LANES if isinstance(at, int) else pl.multiple_of(at * LANES, LANES), count * LANES)
        return [
            pltpu.make_async_remote_copy(
                src_ref=rx.at[lev, :, at],
                dst_ref=rx.at[lev, :, at],
                send_sem=lev_send.at[no, d - 1],
                recv_sem=lev_recv.at[no, d - 1],
                device_id={"lev": lax.rem(lev + d, nlev)},
                device_id_type=MESH,
            )
            for d in range(1, nlev)
        ]

    def arrive(side):
        for copy in halo_copies(side, range(3)):
            copy.wait_recv()
        at = pl.ds(pl.multiple_of(side * (FIELD_HALO + cells), LANES), FIELD_HALO)
        for f in range(3):
            F[f * group : (f + 1) * group, at] = f_halo[side, f]
        for i in range(0, own_lo, 2):
            split_pair(side * own_hi + i, 0)
        for i in range(1, own_lo + 2, 2):
            split_pair(side * (own_hi - 2) + i, 1)
        at = pl.ds(pl.multiple_of(side * (HALO + cells), LANES), HALO)
        shift = HALO + (2 * side - 1) * cells
        si[:, at] = si_halo[side, :, 0, :] + shift
        sw[:, at] = sw_halo[side, :, 0, :]

    def arrive_grid(side):
        for copy in halo_copies(side, range(3, 7)):
            copy.wait_recv()
        at = pl.ds(pl.multiple_of(side * (HALO + cells), LANES), HALO)
        shift = HALO + (2 * side - 1) * cells
        nb[:, at] = nb_halo[side] + (shift - NBR_REACH)
        lw[:, at] = lw_halo[side]
        gx[:, at] = ex_halo[side]
        gy[:, at] = ey_halo[side]

    for copy in loads:
        copy.wait()
    for f in range(3):
        F[f * group : (f + 1) * group, FIELD_HALO : FIELD_HALO + cells] = fields[f]
    own = slice(HALO, HALO + cells)
    si[:, own] = s_index[:, 0, :] + HALO
    sw[:, own] = s_weight[:, 0, :]
    for tile in range(own_lo, own_hi, 2):
        split_pair(tile, 0)
    for tile in range(own_lo + 1, own_hi, 2):
        split_pair(tile, 1)
    nb[:, own] = nbr[...] + (HALO - NBR_REACH)
    lw[:, own] = lap[...]
    gx[:, own] = ex[...]
    gy[:, own] = ey[...]
    middle = first + 2
    for b in range(first, middle):
        upstream(b, b % 2)
        neighbour_matrix(b)

    @pl.when(patch == 0)
    def _():
        pl.semaphore_wait(near_sem, 1)
        start(halo_copies(0))

    for b in range(middle, last):
        upstream(b, b % 2)
        neighbour_matrix(b)

    @pl.when(patch == 0)
    def _():
        pl.semaphore_wait(barrier, 2 + nlev - 2)
        start(halo_copies(1) + helm_copies())

    loop(*inner, right_side, inner[1])
    for copy in lev_copies(0, *inner):
        copy.start()
    begin = 1 - lax.rem(patch, 2)

    def flank(side, turn):
        arrive(side)
        if turn == 0:
            arrive_grid(side)
            for i in range(first):
                upstream(side * last + i, i % 2)
                if i < first - 1:
                    neighbour_matrix(side * (last - 1) + 1 + i)
        else:
            for i in range(hb):
                upstream(side * (nb_blocks - hb) + i, i % 2, by_lane=())
            for m in range(mixed):
                upstream(near(side, m), 0, side * (tiles - 1 - m), m + 1, range(points), True)
            arrive_grid(side)
        loop(side * (last - 1), outer, right_side, outer)
        for copy in lev_copies(1 + turn, side * (last - 1), outer):
            copy.start()
        if turn:
            neighbour_matrix(side * (nb_blocks - 3) + 1)

    mixed = first - hb

    def near(side, m):
        return first - 1 - m + side * (last - first + 1 + 2 * m)

    flank(begin, 0)
    side = 1 - begin
    for m in range(mixed):
        b, t0 = near(side, m), (1 - side) * (m + 1)
        upstream(b, lax.rem(b + t0, 2), t0, tiles - 1 - m)
        neighbour_matrix(b)
    flank(side, 1)

    for f in range(2):
        winds_out[:, f, :] = U[f * group : (f + 1) * group, own]

    for copy in helm_copies():
        copy.wait()
    lrows = up8(levels)
    row = lax.broadcasted_iota(i32, (lrows, group), 0)
    col = lax.broadcasted_iota(i32, (lrows, group), 1)
    c = jnp.zeros((lrows, 1), f32)
    for g in range(nlev):
        c = c + jnp.sum(jnp.where(row - g * group == col, hc[g], 0.0), axis=1, keepdims=True)
    radius = 6.0 * c / (1.0 + 6.0 * c)
    steps = [
        jnp.broadcast_to(
            1.0 / (1.0 + radius * math.cos(math.pi * (2 * j + 1) / (2.0 * SWEEPS))), (lrows, LANES)
        )
        for j in range(SWEEPS)
    ]
    c = jnp.broadcast_to(c, (lrows, LANES))
    nv = lrows // SUB
    to_parts = split(to_modes[...])
    back = from_modes[0:group, :]
    for g in range(1, nlev):
        back = jnp.where(lev == g, from_modes[g * group : (g + 1) * group, :], back)
    back_parts = split(back)

    def modal(b):
        cols = cols_of(b)
        wsum = jnp.sum(lw[:, cols], axis=0, keepdims=True)
        new = []
        total = product(to_parts, jnp.concatenate([rx[g, :, cols] for g in range(nlev)], axis=0))
        for r in range(nv):
            rows = pl.ds(r * SUB, SUB)
            cr = c[r * SUB : (r + 1) * SUB]
            inv = 1.0 / (1.0 + cr * wsum)
            scaled = total[r * SUB : (r + 1) * SUB] * inv
            rinv[rows, cols] = scaled
            cinv[rows, cols] = cr * inv
            new.append(steps[0][r * SUB : (r + 1) * SUB] * scaled)
            xa[rows, cols] = new[r]
        xs0[:, cols] = stack(jnp.concatenate(new, axis=0))

    def stack(x):
        return jnp.concatenate([x, x - x.astype(bf16).astype(f32)], axis=0).astype(bf16)

    def sweep(j, b):
        x_old, x_new = (xa, xb) if j % 2 else (xb, xa)
        cols = cols_of(b)
        s_old, s_new = (xs0, xs1) if j % 2 else (xs1, xs0)
        around_b = jnp.where(
            wide_low, s_old[:, cols_of(jnp.minimum(b + 1, nb_blocks - 1))], s_old[:, cols_of(jnp.maximum(b - 1, 0))]
        )
        got = jnp.dot(
            jnp.concatenate([s_old[:, cols], around_b], axis=1), L[b], preferred_element_type=f32
        )
        acc = (got[0:lrows, 0:LANES] + got[0:lrows, LANES:]) + (got[lrows:, 0:LANES] + got[lrows:, LANES:])
        new = []
        for r in range(nv):
            rows = pl.ds(r * SUB, SUB)
            s = steps[j][r * SUB : (r + 1) * SUB]
            new.append((1.0 - s) * x_old[rows, cols] + s * (
                rinv[rows, cols] + cinv[rows, cols] * acc[r * SUB : (r + 1) * SUB]
            ))
            x_new[rows, cols] = new[r]
        if j < SWEEPS - 1:
            s_new[:, cols] = stack(jnp.concatenate(new, axis=0))

    wide_low = lax.broadcasted_iota(i32, (2 * lrows, LANES), 1).astype(f32).astype(bf16) < NBR_REACH

    x_end = xa if SWEEPS % 2 else xb

    def heights(b):
        height_out[:, cols_of(b - hb)] = product(back_parts, x_end[0:levels, cols_of(b)])

    def off(j):
        return hb - -(-(NBR_REACH * (SWEEPS - 1 - j)) // LANES)

    def finish(side, first_part):
        def part(at, j):
            width = nb_blocks - outer if first_part else outer
            low = (nb_blocks - width) * side
            if j == 0:
                return low, width
            grow = -j if first_part else j
            width = width + grow - at
            return low + jnp.where(side == 0, at, -grow), width

        many = 1 if nv > 4 else nb_blocks
        loop(*part(0, 0), modal, min(many, part(0, 0)[1]))
        for j in range(1, SWEEPS):
            start, count = part(off(j), j)
            loop(start, count, functools.partial(sweep, j), min(many, count))
        start, count = part(hb, SWEEPS - 1)
        loop(start, count, heights, count)

    for copy in lev_copies(0, *inner) + lev_copies(1, begin * (last - 1), outer):
        copy.wait_recv()
    finish(begin, True)
    for copy in lev_copies(2, (1 - begin) * (last - 1), outer):
        copy.wait_recv()
    finish(1 - begin, False)
    for side in (0, 1):
        for copy in halo_copies(side):
            copy.wait_send()
    for copy in lev_copies(0, *inner):
        copy.wait_send()
    for no in (1, 2):
        for copy in lev_copies(no, 0, outer):
            copy.wait_send()


def hand_over(winds_in, height_in, winds_out, height_out, sem):
    copies = [
        pltpu.make_async_copy(winds_in, winds_out, sem.at[0]),
        pltpu.make_async_copy(height_in, height_out, sem.at[1]),
    ]
    for copy in copies:
        copy.start()
    for copy in copies:
        copy.wait()


def per_device(npatch, nlev, *args):
    fields, s_index, _, nbr = args[:4]
    _, group, cells = fields.shape
    points, sides = s_index.shape[0], nbr.shape[0]
    levels = group * nlev
    ext = cells + 2 * HALO
    args = args[:-1] + (args[-1].reshape(1, group),)
    args = [pltpu.with_memory_space_constraint(a, pltpu.HBM) for a in args]
    lrows = up8(levels)
    vm = pltpu.VMEM
    peers = max(nlev - 1, 1)
    winds, height = pl.pallas_call(
        functools.partial(kernel, npatch, nlev),
        out_shape=(
            pltpu.VMEM((group, 2, cells), f32),
            pltpu.VMEM((group, cells), f32),
        ),
        in_specs=[pl.BlockSpec(memory_space=pl.ANY)] * 7
        + [pl.BlockSpec(memory_space=pltpu.VMEM)] * 3,
        out_specs=(
            pl.BlockSpec(memory_space=pltpu.VMEM),
            pl.BlockSpec(memory_space=pltpu.VMEM),
        ),
        scratch_shapes=[vm(a.shape, a.dtype) for a in args[:7]]
        + [
            pltpu.SemaphoreType.DMA((7,)),
            vm((2, 3, group, FIELD_HALO), f32),
            vm((2, points, 1, HALO), i32),
            vm((2, points, 1, HALO), f32),
            vm((2, sides, HALO), i32),
            vm((2, sides, HALO), f32),
            vm((2, sides, HALO), f32),
            vm((2, sides, HALO), f32),
            vm((nlev, 1, group), f32),
            vm((up8(3 * group), cells + 2 * FIELD_HALO + LANES), f32),
            vm((2 * up8(3 * group) * ((cells + 2 * FIELD_HALO) // LANES + 2), 2 * LANES), bf16),
            vm((ext // LANES, 2 * LANES, 2 * LANES), bf16),
            vm((points, ext), i32),
            vm((points, ext), f32),
            vm((sides, ext), i32),
            vm((sides, ext), f32),
            vm((sides, ext), f32),
            vm((sides, ext), f32),
            vm((up8(3 * group), ext), f32),
            vm((nlev, group, ext), f32),
            vm((lrows, ext), f32),
            vm((lrows, ext), f32),
            vm((lrows, ext), f32),
            vm((lrows, ext), f32),
            vm((2 * lrows, ext), bf16),
            vm((2 * lrows, ext), bf16),
            pltpu.SemaphoreType.REGULAR,
            pltpu.SemaphoreType.DMA((14,)),
            pltpu.SemaphoreType.DMA((14,)),
            pltpu.SemaphoreType.DMA((3, peers)),
            pltpu.SemaphoreType.DMA((3, peers)),
            pltpu.SemaphoreType.DMA((peers,)),
            pltpu.SemaphoreType.DMA((peers,)),
        ],
        compiler_params=pltpu.CompilerParams(
            collective_id=0, has_side_effects=True, vmem_limit_bytes=20 << 20
        ),
    )(*args)
    winds, height = pl.pallas_call(
        hand_over,
        out_shape=(
            jax.ShapeDtypeStruct(winds.shape, f32),
            jax.ShapeDtypeStruct(height.shape, f32),
        ),
        in_specs=[pl.BlockSpec(memory_space=pltpu.VMEM)] * 2,
        out_specs=(pl.BlockSpec(memory_space=pl.ANY),) * 2,
        scratch_shapes=[pltpu.SemaphoreType.DMA((2,))],
        compiler_params=pltpu.CompilerParams(vmem_limit_bytes=1 << 20),
    )(winds, height)
    return jnp.transpose(winds, (1, 0, 2)), height


def solution(mesh):
    in_specs = (
        P(None, "lev", "patch"),
        P(None, "lev", "patch"),
        P(None, "lev", "patch"),
        P(None, "patch"),
        P(None, "patch"),
        P(None, "patch"),
        P(None, "patch"),
        P(),
        P(),
        P("lev"),
    )
    out_specs = (P(None, "lev", "patch"), P("lev", "patch"))
    body = functools.partial(per_device, mesh.shape["patch"], mesh.shape["lev"])
    return jax.shard_map(
        body, mesh=mesh, in_specs=in_specs, out_specs=out_specs, check_vma=False
    )
```

```python
import functools
import math

import jax
import jax.numpy as jnp
from jax import lax
from jax.experimental import pallas as pl
from jax.experimental.pallas import tpu as pltpu
from jax.sharding import PartitionSpec as P

REACH = 512
NBR_REACH = 64
SWEEPS = 4
COUPLING = 0.5
LANES = 128
SUB = 8
HALO = NBR_REACH * SWEEPS
FIELD_HALO = REACH + HALO
MESH = pl.DeviceIdType.MESH


BITS = LANES.bit_length() - 1
bf16, f32, i32 = jnp.bfloat16, jnp.float32, jnp.int32


def up8(rows):
    return -(-rows // SUB) * SUB


def split(x):
    high = x.astype(bf16)
    return high, (x - high.astype(f32)).astype(bf16)


def product(parts, x):
    high, low = split(x)
    dot = functools.partial(jnp.dot, preferred_element_type=f32)
    return dot(parts[0], high) + (dot(parts[1], high) + dot(parts[0], low))


def lanes_of(x, index):
    return jnp.take_along_axis(x, index, axis=1, mode="promise_in_bounds")


def row8(ref, row, cols):
    return jnp.broadcast_to(ref[pl.ds(row, 1), cols], (SUB, LANES))


def cols_of(block):
    if isinstance(block, int):
        return slice(block * LANES, (block + 1) * LANES)
    return pl.ds(pl.multiple_of(block * LANES, LANES), LANES)


def loop(first, count, body, unroll=1):
    trips = count // unroll

    def step(i, carry):
        for u in range(unroll):
            body(first + i * unroll + u)
        return carry

    if trips == 1:
        step(0, 0)
    else:
        lax.fori_loop(0, trips, step, 0)
    for u in range(trips * unroll, count):
        body(first + u)


def kernel(
    npatch, nlev,
    fields_in, s_index_in, s_weight_in, nbr_in, lap_in, ex_in, ey_in, to_modes, from_modes, helm,
    winds_out, height_out,
    fields, s_index, s_weight, nbr, lap, ex, ey, load_sem,
    f_halo, si_halo, sw_halo, nb_halo, lw_halo, ex_halo, ey_halo, hc,
    F, G, L, si, sw, nb, lw, gx, gy, U, rx, rinv, cinv, xa, xb, xs0, xs1,
    near_sem, send_sem, recv_sem, lev_send, lev_recv, hc_send, hc_recv,
):
    group = fields.shape[1]
    cells = fields.shape[2]
    levels = group * nlev
    points = s_index.shape[0]
    sides = nbr.shape[0]
    ext = cells + 2 * HALO
    nb_blocks = ext // LANES
    own_blocks = cells // LANES
    hb = HALO // LANES
    patch = lax.axis_index("patch")
    lev = lax.axis_index("lev")
    right = lax.rem(patch + 1, npatch)
    left = lax.rem(patch + npatch - 1, npatch)

    barrier = pltpu.get_barrier_semaphore()
    pl.semaphore_signal(barrier, inc=1, device_id={"patch": right}, device_id_type=MESH)

    @pl.when(patch != 1)
    def _():
        pl.semaphore_signal(barrier, inc=1, device_id={"patch": left}, device_id_type=MESH)

    for d in range(1, nlev):
        pl.semaphore_signal(
            barrier, inc=1, device_id={"lev": lax.rem(lev + d, nlev)}, device_id_type=MESH
        )
    loads = []
    for no, (src, dst) in enumerate((
        (fields_in, fields), (s_index_in, s_index), (s_weight_in, s_weight),
        (nbr_in, nbr), (lap_in, lap), (ex_in, ex), (ey_in, ey),
    )):
        copy = pltpu.make_async_copy(src, dst, load_sem.at[no])
        copy.start()
        loads.append(copy)
    hc[lev] = helm[...]

    pairs = (
        (s_index_in, si_halo, HALO),
        (s_weight_in, sw_halo, HALO),
        (fields_in, f_halo, FIELD_HALO),
        (nbr_in, nb_halo, HALO),
        (ex_in, ex_halo, HALO),
        (ey_in, ey_halo, HALO),
        (lap_in, lw_halo, HALO),
    )

    def halo_copies(side, kinds=range(7)):
        made = []
        for no in kinds:
            src, dst, width = pairs[no]
            lead = (slice(None),) * (len(src.shape) - 1)
            start = (1 - side) * (cells - width)
            if not isinstance(side, int):
                start = pl.multiple_of(start, LANES)
            made.append(pltpu.make_async_remote_copy(
                src_ref=src.at[lead + (pl.ds(start, width),)],
                dst_ref=dst.at[side],
                send_sem=send_sem.at[2 * no + side],
                recv_sem=recv_sem.at[2 * no + side],
                device_id={"patch": lax.rem(patch + npatch + 1 - 2 * side, npatch)},
                device_id_type=MESH,
            ))
        return made

    def helm_copies():
        return [
            pltpu.make_async_remote_copy(
                src_ref=helm,
                dst_ref=hc.at[lev],
                send_sem=hc_send.at[d - 1],
                recv_sem=hc_recv.at[d - 1],
                device_id={"lev": lax.rem(lev + d, nlev)},
                device_id_type=MESH,
            )
            for d in range(1, nlev)
        ]

    def start(made):
        for copy in made:
            copy.start()

    @pl.when(patch != 0)
    def _():
        pl.semaphore_wait(barrier, 2 + nlev - 1)

    @pl.when(patch == 1)
    def _():
        pl.semaphore_signal(near_sem, inc=1, device_id={"patch": left}, device_id_type=MESH)

    @pl.when(patch != 0)
    def _():
        start(halo_copies(0) + halo_copies(1) + helm_copies())

    frows = F.shape[0]
    tiles = 2 * REACH // LANES + 1
    ftiles = F.shape[1] // LANES
    own_lo = FIELD_HALO // LANES
    own_hi = own_lo + own_blocks

    def tile_rows(tile, count, odd):
        start = tile * frows + odd * (G.shape[0] // 2 + frows % (2 * SUB))
        if not isinstance(start, int):
            start = pl.multiple_of(start, 2 * SUB)
        return pl.ds(start, count * frows)

    def split_pair(tile, odd):
        rows = tile_rows(tile, 2, odd)
        high, low = split(
            jnp.concatenate([F[:, cols_of(tile)], F[:, cols_of(tile + 1)]], axis=0)
        )
        G[rows, 0:LANES] = high
        G[rows, LANES : 2 * LANES] = low

    lane_id = lax.broadcasted_iota(i32, (LANES, LANES), 0).astype(f32).astype(bf16)
    one = jnp.ones((LANES, LANES), bf16)
    zero = jnp.zeros((LANES, LANES), bf16)

    def upstream(b, odd, t0=0, count=tiles, by_lane=(2, 5), add=False):
        cols = cols_of(b)
        nv = frows // SUB
        acc = [None] * nv
        field = G.at[tile_rows(b + t0, count, odd), :]
        for pair_no in range(points // 2):
            pair = (2 * pair_no, 2 * pair_no + 1)
            his, los = [], []
            for q in pair:
                x = row8(si, q, cols)
                his.append((x >> BITS) - b)
                los.append(x & (LANES - 1))
            on_lanes = pair_no in by_lane
            if not on_lanes:
                got = jnp.dot(field[...], one_hot(los), preferred_element_type=f32)
            for no, q in enumerate(pair):
                w = row8(sw, q, cols)
                here = [his[no] - t0 == t for t in range(count)]
                for r in range(nv):
                    sel = None if count == tiles else jnp.zeros((SUB, LANES), f32)
                    for t in range(count):
                        row = t * frows + r * SUB
                        if on_lanes:
                            taken = lanes_of(
                                F[r * SUB : (r + 1) * SUB, cols_of(b + t0 + t)], los[no]
                            )
                        else:
                            taken = got[row : row + SUB, no * LANES : (no + 1) * LANES]
                        sel = taken if sel is None else jnp.where(here[t], taken, sel)
                    acc[r] = w * sel if acc[r] is None else acc[r] + w * sel
        for r in range(nv):
            at = slice(r * SUB, (r + 1) * SUB)
            U[at, cols] = U[at, cols] + acc[r] if add else acc[r]

    lane = lax.broadcasted_iota(i32, (SUB, LANES), 1)
    low_half = lane < NBR_REACH

    def around(ref, b, nvregs):
        before = jnp.maximum(b - 1, 0)
        after = jnp.minimum(b + 1, nb_blocks - 1)
        own_tiles, far_tiles = [], []
        for r in range(nvregs):
            rows = pl.ds(r * SUB, SUB)
            own_tiles.append(ref[rows, cols_of(b)])
            far_tiles.append(
                jnp.where(low_half, ref[rows, cols_of(after)], ref[rows, cols_of(before)])
            )
        return own_tiles, far_tiles

    def place(k, b, cols):
        x = row8(nb, k, cols)
        return x & (LANES - 1), (x >> BITS) == b

    window_id = lax.broadcasted_iota(i32, (2 * LANES, LANES), 0).astype(f32).astype(bf16)

    def wide(x):
        return jnp.broadcast_to(x[0:1], (2 * LANES, LANES)).astype(bf16)

    def neighbour_matrix(b):
        cols = cols_of(b)
        at, weight = [], []
        for q in range(sides):
            lo, here = place(q, b, cols)
            at.append(jnp.where(here, lo, lo + LANES))
            weight.append(row8(lw, q, cols))
        for q in range(sides):
            for p in range(q + 1, sides):
                weight[q] = weight[q] + jnp.where(at[q] == at[p], row8(lw, p, cols), 0.0)
        high = jnp.zeros((2 * LANES, LANES), bf16)
        low = jnp.zeros((2 * LANES, LANES), bf16)
        for q in reversed(range(sides)):
            w_high = weight[q].astype(bf16).astype(f32)
            hit = window_id == wide(at[q].astype(f32))
            high = jnp.where(hit, wide(w_high), high)
            low = jnp.where(hit, wide(weight[q] - w_high), low)
        L[b, :, 0:LANES] = high
        L[b, :, LANES : 2 * LANES] = low

    def one_hot(los):
        hot = []
        for lo in los:
            lo = jnp.broadcast_to(lo[0:1].astype(f32), (LANES, LANES))
            h = jnp.where(lane_id == lo.astype(bf16), one, zero)
            hot.append(jnp.concatenate([h, h], axis=0))
        return jnp.concatenate(hot, axis=1)

    def beside(own_t, far_t, b, cols):
        nv = len(own_t)
        places = [place(k, b, cols) for k in range(sides)]
        by_product = range(sides - 2, sides)
        if len(by_product):
            high, low = split(jnp.concatenate(own_t + far_t, axis=0))
            got = jnp.dot(
                jnp.concatenate([high, low], axis=1),
                one_hot([places[k][0] for k in by_product]),
                preferred_element_type=f32,
            )
        for k in range(sides):
            lo, here = places[k]
            for r in range(nv):
                if k in by_product:
                    at = (k - by_product[0]) * LANES
                    mine = got[r * SUB : (r + 1) * SUB, at : at + LANES]
                    far = got[(nv + r) * SUB : (nv + r + 1) * SUB, at : at + LANES]
                else:
                    mine, far = lanes_of(own_t[r], lo), lanes_of(far_t[r], lo)
                yield k, r, jnp.where(here, mine, far)

    wrows = up8(2 * group)
    sub_iota = lax.broadcasted_iota(i32, (SUB, LANES), 0)

    def right_side(b):
        cols = cols_of(b)
        nv = wrows // SUB
        own_t, far_t = around(U, b, nv)
        acc = [jnp.zeros((SUB, LANES), f32)] * nv
        for k, r, taken in beside(own_t, far_t, b, cols):
            wx, wy = row8(gx, k, cols), row8(gy, k, cols)
            if (r + 1) * SUB <= group:
                w = wx
            elif r * SUB >= group:
                w = wy
            else:
                w = jnp.where(sub_iota + r * SUB < group, wx, wy)
            acc[r] = acc[r] + w * (taken - own_t[r])
        both = jnp.concatenate(acc, axis=0)
        div = both[0:group] + both[group : 2 * group]
        rx[lev, :, cols] = U[2 * group : 3 * group, cols] - COUPLING * div

    first = hb + REACH // LANES
    last = nb_blocks - first
    inner = (first + 1, last - first - 2)
    outer = first + 1

    def lev_copies(no, at, count):
        at = pl.ds(at * LANES if isinstance(at, int) else pl.multiple_of(at * LANES, LANES), count * LANES)
        return [
            pltpu.make_async_remote_copy(
                src_ref=rx.at[lev, :, at],
                dst_ref=rx.at[lev, :, at],
                send_sem=lev_send.at[no, d - 1],
                recv_sem=lev_recv.at[no, d - 1],
                device_id={"lev": lax.rem(lev + d, nlev)},
                device_id_type=MESH,
            )
            for d in range(1, nlev)
        ]

    def arrive(side):
        for copy in halo_copies(side, range(3)):
            copy.wait_recv()
        at = pl.ds(pl.multiple_of(side * (FIELD_HALO + cells), LANES), FIELD_HALO)
        for f in range(3):
            F[f * group : (f + 1) * group, at] = f_halo[side, f]
        for i in range(0, own_lo, 2):
            split_pair(side * own_hi + i, 0)
        for i in range(1, own_lo + 2, 2):
            split_pair(side * (own_hi - 2) + i, 1)
        at = pl.ds(pl.multiple_of(side * (HALO + cells), LANES), HALO)
        shift = HALO + (2 * side - 1) * cells
        si[:, at] = si_halo[side, :, 0, :] + shift
        sw[:, at] = sw_halo[side, :, 0, :]

    def arrive_grid(side):
        for copy in halo_copies(side, range(3, 7)):
            copy.wait_recv()
        at = pl.ds(pl.multiple_of(side * (HALO + cells), LANES), HALO)
        shift = HALO + (2 * side - 1) * cells
        nb[:, at] = nb_halo[side] + (shift - NBR_REACH)
        lw[:, at] = lw_halo[side]
        gx[:, at] = ex_halo[side]
        gy[:, at] = ey_halo[side]

    for copy in loads:
        copy.wait()
    for f in range(3):
        F[f * group : (f + 1) * group, FIELD_HALO : FIELD_HALO + cells] = fields[f]
    own = slice(HALO, HALO + cells)
    si[:, own] = s_index[:, 0, :] + HALO
    sw[:, own] = s_weight[:, 0, :]
    for tile in range(own_lo, own_hi, 2):
        split_pair(tile, 0)
    for tile in range(own_lo + 1, own_hi, 2):
        split_pair(tile, 1)
    nb[:, own] = nbr[...] + (HALO - NBR_REACH)
    lw[:, own] = lap[...]
    gx[:, own] = ex[...]
    gy[:, own] = ey[...]
    middle = first + 2
    for b in range(first, middle):
        upstream(b, b % 2)
        neighbour_matrix(b)

    @pl.when(patch == 0)
    def _():
        pl.semaphore_wait(near_sem, 1)
        start(halo_copies(0))

    for b in range(middle, last):
        upstream(b, b % 2)
        neighbour_matrix(b)

    @pl.when(patch == 0)
    def _():
        pl.semaphore_wait(barrier, 2 + nlev - 2)
        start(halo_copies(1) + helm_copies())

    loop(*inner, right_side, inner[1])
    for copy in lev_copies(0, *inner):
        copy.start()
    early = (outer + 1) // 2
    pieces = (((1, 0, outer),), ((2, 0, early), (3, early, outer - early)))
    begin = 1 - lax.rem(patch, 2)

    def flank(side, turn):
        arrive(side)
        if turn == 0:
            arrive_grid(side)
            for i in range(first):
                upstream(side * last + i, i % 2)
                if i < first - 1:
                    neighbour_matrix(side * (last - 1) + 1 + i)
        else:
            for i in range(hb):
                upstream(side * (nb_blocks - hb) + i, i % 2, by_lane=())
            for m in range(mixed):
                upstream(near(side, m), 0, side * (tiles - 1 - m), m + 1, range(points), True)
            arrive_grid(side)
        at = side * (last - 1)
        for no, skip, count in pieces[turn]:
            loop(at + skip, count, right_side, count)
            for copy in lev_copies(no, at + skip, count):
                copy.start()
        if turn:
            neighbour_matrix(side * (nb_blocks - 3) + 1)

    mixed = first - hb

    def near(side, m):
        return first - 1 - m + side * (last - first + 1 + 2 * m)

    flank(begin, 0)
    side = 1 - begin
    for m in range(mixed):
        b, t0 = near(side, m), (1 - side) * (m + 1)
        upstream(b, lax.rem(b + t0, 2), t0, tiles - 1 - m)
        neighbour_matrix(b)
    flank(side, 1)

    for f in range(2):
        winds_out[:, f, :] = U[f * group : (f + 1) * group, own]

    for copy in helm_copies():
        copy.wait()
    lrows = up8(levels)
    row = lax.broadcasted_iota(i32, (lrows, group), 0)
    col = lax.broadcasted_iota(i32, (lrows, group), 1)
    c = jnp.zeros((lrows, 1), f32)
    for g in range(nlev):
        c = c + jnp.sum(jnp.where(row - g * group == col, hc[g], 0.0), axis=1, keepdims=True)
    radius = 6.0 * c / (1.0 + 6.0 * c)
    steps = [
        jnp.broadcast_to(
            1.0 / (1.0 + radius * math.cos(math.pi * (2 * j + 1) / (2.0 * SWEEPS))), (lrows, LANES)
        )
        for j in range(SWEEPS)
    ]
    c = jnp.broadcast_to(c, (lrows, LANES))
    nv = lrows // SUB
    to_parts = split(to_modes[...])
    back = from_modes[0:group, :]
    for g in range(1, nlev):
        back = jnp.where(lev == g, from_modes[g * group : (g + 1) * group, :], back)
    back_parts = split(back)

    def modal(b):
        cols = cols_of(b)
        wsum = jnp.sum(lw[:, cols], axis=0, keepdims=True)
        new = []
        total = product(to_parts, jnp.concatenate([rx[g, :, cols] for g in range(nlev)], axis=0))
        for r in range(nv):
            rows = pl.ds(r * SUB, SUB)
            cr = c[r * SUB : (r + 1) * SUB]
            inv = 1.0 / (1.0 + cr * wsum)
            scaled = total[r * SUB : (r + 1) * SUB] * inv
            rinv[rows, cols] = scaled
            cinv[rows, cols] = cr * inv
            new.append(steps[0][r * SUB : (r + 1) * SUB] * scaled)
            xa[rows, cols] = new[r]
        xs0[:, cols] = stack(jnp.concatenate(new, axis=0))

    def stack(x):
        return jnp.concatenate([x, x - x.astype(bf16).astype(f32)], axis=0).astype(bf16)

    def sweep(j, b):
        x_old, x_new = (xa, xb) if j % 2 else (xb, xa)
        cols = cols_of(b)
        s_old, s_new = (xs0, xs1) if j % 2 else (xs1, xs0)
        around_b = jnp.where(
            wide_low, s_old[:, cols_of(jnp.minimum(b + 1, nb_blocks - 1))], s_old[:, cols_of(jnp.maximum(b - 1, 0))]
        )
        got = jnp.dot(
            jnp.concatenate([s_old[:, cols], around_b], axis=1), L[b], preferred_element_type=f32
        )
        acc = (got[0:lrows, 0:LANES] + got[0:lrows, LANES:]) + (got[lrows:, 0:LANES] + got[lrows:, LANES:])
        new = []
        for r in range(nv):
            rows = pl.ds(r * SUB, SUB)
            s = steps[j][r * SUB : (r + 1) * SUB]
            new.append((1.0 - s) * x_old[rows, cols] + s * (
                rinv[rows, cols] + cinv[rows, cols] * acc[r * SUB : (r + 1) * SUB]
            ))
            x_new[rows, cols] = new[r]
        if j < SWEEPS - 1:
            s_new[:, cols] = stack(jnp.concatenate(new, axis=0))

    wide_low = lax.broadcasted_iota(i32, (2 * lrows, LANES), 1).astype(f32).astype(bf16) < NBR_REACH

    x_end = xa if SWEEPS % 2 else xb

    def heights(b):
        height_out[:, cols_of(b - hb)] = product(back_parts, x_end[0:levels, cols_of(b)])

    def off(j):
        return hb - -(-(NBR_REACH * (SWEEPS - 1 - j)) // LANES)

    def finish(side, first_part):
        def part(at, j):
            width = nb_blocks - outer if first_part else outer
            low = (nb_blocks - width) * side
            if j == 0:
                return low, width
            grow = -j if first_part else j
            width = width + grow - at
            return low + jnp.where(side == 0, at, -grow), width

        many = 1 if nv > 4 else nb_blocks
        loop(*part(0, 0), modal, min(many, part(0, 0)[1]))
        for j in range(1, SWEEPS):
            start, count = part(off(j), j)
            loop(start, count, functools.partial(sweep, j), min(many, count))
        start, count = part(hb, SWEEPS - 1)
        loop(start, count, heights, count)

    for copy in lev_copies(0, *inner) + lev_copies(1, begin * (last - 1), outer):
        copy.wait_recv()
    finish(begin, True)
    for no, skip, count in pieces[1]:
        for copy in lev_copies(no, (1 - begin) * (last - 1) + skip, count):
            copy.wait_recv()
    finish(1 - begin, False)
    for side in (0, 1):
        for copy in halo_copies(side):
            copy.wait_send()
    for copy in lev_copies(0, *inner):
        copy.wait_send()
    for no, skip, count in pieces[0] + pieces[1]:
        for copy in lev_copies(no, skip, count):
            copy.wait_send()


def hand_over(winds_in, height_in, winds_out, height_out, sem):
    copies = [
        pltpu.make_async_copy(winds_in, winds_out, sem.at[0]),
        pltpu.make_async_copy(height_in, height_out, sem.at[1]),
    ]
    for copy in copies:
        copy.start()
    for copy in copies:
        copy.wait()


def per_device(npatch, nlev, *args):
    fields, s_index, _, nbr = args[:4]
    _, group, cells = fields.shape
    points, sides = s_index.shape[0], nbr.shape[0]
    levels = group * nlev
    ext = cells + 2 * HALO
    args = args[:-1] + (args[-1].reshape(1, group),)
    args = [pltpu.with_memory_space_constraint(a, pltpu.HBM) for a in args]
    lrows = up8(levels)
    vm = pltpu.VMEM
    peers = max(nlev - 1, 1)
    winds, height = pl.pallas_call(
        functools.partial(kernel, npatch, nlev),
        out_shape=(
            pltpu.VMEM((group, 2, cells), f32),
            pltpu.VMEM((group, cells), f32),
        ),
        in_specs=[pl.BlockSpec(memory_space=pl.ANY)] * 7
        + [pl.BlockSpec(memory_space=pltpu.VMEM)] * 3,
        out_specs=(
            pl.BlockSpec(memory_space=pltpu.VMEM),
            pl.BlockSpec(memory_space=pltpu.VMEM),
        ),
        scratch_shapes=[vm(a.shape, a.dtype) for a in args[:7]]
        + [
            pltpu.SemaphoreType.DMA((7,)),
            vm((2, 3, group, FIELD_HALO), f32),
            vm((2, points, 1, HALO), i32),
            vm((2, points, 1, HALO), f32),
            vm((2, sides, HALO), i32),
            vm((2, sides, HALO), f32),
            vm((2, sides, HALO), f32),
            vm((2, sides, HALO), f32),
            vm((nlev, 1, group), f32),
            vm((up8(3 * group), cells + 2 * FIELD_HALO + LANES), f32),
            vm((2 * up8(3 * group) * ((cells + 2 * FIELD_HALO) // LANES + 2), 2 * LANES), bf16),
            vm((ext // LANES, 2 * LANES, 2 * LANES), bf16),
            vm((points, ext), i32),
            vm((points, ext), f32),
            vm((sides, ext), i32),
            vm((sides, ext), f32),
            vm((sides, ext), f32),
            vm((sides, ext), f32),
            vm((up8(3 * group), ext), f32),
            vm((nlev, group, ext), f32),
            vm((lrows, ext), f32),
            vm((lrows, ext), f32),
            vm((lrows, ext), f32),
            vm((lrows, ext), f32),
            vm((2 * lrows, ext), bf16),
            vm((2 * lrows, ext), bf16),
            pltpu.SemaphoreType.REGULAR,
            pltpu.SemaphoreType.DMA((14,)),
            pltpu.SemaphoreType.DMA((14,)),
            pltpu.SemaphoreType.DMA((4, peers)),
            pltpu.SemaphoreType.DMA((4, peers)),
            pltpu.SemaphoreType.DMA((peers,)),
            pltpu.SemaphoreType.DMA((peers,)),
        ],
        compiler_params=pltpu.CompilerParams(
            collective_id=0, has_side_effects=True, vmem_limit_bytes=20 << 20
        ),
    )(*args)
    winds, height = pl.pallas_call(
        hand_over,
        out_shape=(
            jax.ShapeDtypeStruct(winds.shape, f32),
            jax.ShapeDtypeStruct(height.shape, f32),
        ),
        in_specs=[pl.BlockSpec(memory_space=pltpu.VMEM)] * 2,
        out_specs=(pl.BlockSpec(memory_space=pl.ANY),) * 2,
        scratch_shapes=[pltpu.SemaphoreType.DMA((2,))],
        compiler_params=pltpu.CompilerParams(vmem_limit_bytes=1 << 20),
    )(winds, height)
    return jnp.transpose(winds, (1, 0, 2)), height


def solution(mesh):
    in_specs = (
        P(None, "lev", "patch"),
        P(None, "lev", "patch"),
        P(None, "lev", "patch"),
        P(None, "patch"),
        P(None, "patch"),
        P(None, "patch"),
        P(None, "patch"),
        P(),
        P(),
        P("lev"),
    )
    out_specs = (P(None, "lev", "patch"), P("lev", "patch"))
    body = functools.partial(per_device, mesh.shape["patch"], mesh.shape["lev"])
    return jax.shard_map(
        body, mesh=mesh, in_specs=in_specs, out_specs=out_specs, check_vma=False
    )
```
